32 devices in a mesh: gx: 8 (over z, x), gy: 4 (over y, core).
Axes of the slice: x: 2, y: 2, z: 4, core: 2. Of those that a mesh axis runs over, the one named last changes fastest.
Arguments:
- parcel_props: float32 [16, 131072], P(None, ('gx', 'gy')), may hold values from -6 to 6
- size_class: int32 [131072], P(('gx', 'gy')), may hold values from 0 to 7
- dest_owner: int32 [131072, 1], P(('gx', 'gy')), may hold values from 0 to 31; in each aligned block of 4096 rows (0 to 4095, 4096 to 8191, ...) at most 512 rows name the same one
- dest_local: int32 [131072], P(('gx', 'gy')), may hold values from 0 to 4095
- class_table: float32 [8, 16], replicated, may hold values from 0.5 to 2
- gas_density: float32 [256, 512], P('gx', 'gy'), may hold values from 0.5 to 2
- gas_rest: float32 [4, 256, 512], P(None, 'gx', 'gy'), may hold values from -6 to 6
Outputs:
- new_density: float32 [256, 512], P('gx', 'gy')
- new_rest: float32 [4, 256, 512], P(None, 'gx', 'gy')
The draws below stay inside these ranges and needn't reach their ends.
Inputs may be any that keep to these rules, and one draw needn't show every extreme that they name: `dest_owner`: among the parcels of one device, no owner device is named by more than 512 of them, a bound that some block reaches.
All inputs are finite; a program needn't handle non-finite values.
Results may differ from the reference program's by a relative error of at most 0.00015.
Values sent between devices are 32-bit elements; how exact they have to be, the bound alone decides.
A program may use at most 64 MiB of HBM per device.

```python
import math
import jax
import jax.numpy as jnp
import numpy as np
from jax import lax

PROPS = 16
CLASSES = 8
PARC_DEV = 4096
LX = 32
LY = 128
CAP = 512
PARCELS = 131072
NX = 256
NY = 512
N_GY = 4
DEVICES = 32


def place_ends(drawn, rng, least, high):
    longest = drawn.shape.index(max(drawn.shape))
    spots = []
    for shift in (0, 1):
        where = [jax.random.randint(jax.random.fold_in(rng, axis), (), 0, length) for axis, length in enumerate(drawn.shape)]
        where[longest] = (where[longest] + shift) % drawn.shape[longest]
        spots.append(tuple(where))
    return drawn.at[spots[0]].set(least).at[spots[1]].set(high)


def steps_of(own_key, shape, shards, least, largest):
    def one(axis_at, shards_of):
        heights = jax.random.uniform(jax.random.fold_in(jax.random.fold_in(own_key, 6), axis_at), (shards_of,), jnp.float32, least / len(shards), largest / len(shards))
        return jnp.repeat(jnp.exp(heights), shape[axis_at] // shards_of).reshape((-1,) + (1,) * (len(shape) - axis_at - 1))

    level = one(*shards[0])
    for cut in shards[1:]:
        level = level * one(*cut)
    return level


def routed_block(key, own, number, rows, count, top, limit, lean):
    sequence = jax.random.permutation(key, count)
    packed, common = load_shares(count, rows * top, limit, lean, True), load_shares(count, rows * top, limit, lean, False)
    places = jnp.arange(count)

    def named(tallies, rotation):
        used = int((tallies > 0).sum())
        fixed = max(1, used // 4)
        shifted = fixed + (places - fixed + rotation * (used - fixed)) % max(1, count - fixed)
        return jnp.zeros((count,), jnp.int32).at[sequence[jnp.where(places < fixed, places, shifted)]].set(jnp.asarray(tallies, jnp.int32))

    tallies = jnp.where(number % 4 == 0, named(packed, number // 4), named(common, number - number // 4 - 1))
    mixed = jax.random.permutation(jax.random.fold_in(own, 3), count)
    source_of, sink = mixed[0:count // 2 * 2:2], mixed[1:count // 2 * 2:2]
    margin = jnp.minimum(tallies[source_of] - 1, limit - tallies[sink]) // 2
    margin = jnp.where((source_of == sequence[0]) | (sink == sequence[0]) | (tallies[sink] == 0), 0, jnp.maximum(margin, 0))
    shifted = jax.random.randint(jax.random.fold_in(own, 4), (count // 2,), 0, 1 << 20) % (margin + 1)
    tallies = tallies.at[source_of].add(-shifted).at[sink].add(shifted)
    members = jnp.searchsorted(jnp.cumsum(tallies), jnp.arange(rows * top), side="right").astype(jnp.int32)
    table = members.reshape(top, rows).T
    table = table[jax.random.permutation(jax.random.fold_in(own, 1), rows)]
    rotation = jax.random.randint(jax.random.fold_in(own, 2), (rows, 1), 0, top)
    return jnp.take_along_axis(table, (jnp.arange(top)[None, :] + rotation) % top, axis=1)


def load_shares(count, total, most, lean, full):
    weights = [(1 << 20) // math.isqrt(standing ** lean) + 1 for standing in range(1, count + 1)]
    largest = most if full else min(most, max(-(-total // count), total * weights[0] // sum(weights)))
    least = 1 if total - largest >= count - 1 else 0
    holding, surplus = [largest] + [least] * (count - 1), total - largest - least * (count - 1)
    while surplus > 0:
        free = [i for i in range(1, count) if holding[i] < largest] or [i for i in range(1, count) if holding[i] < most]
        whole, left = sum([weights[i] for i in free]), surplus
        for i in free:
            more = min(most - holding[i], max(1, left * weights[i] // whole), surplus)
            holding[i] = holding[i] + more
            surplus = surplus - more
    return np.array(holding)


def bell_draw(key, extent, width, most, cuts=(), kind=jnp.bfloat16):
    array = width * jax.random.normal(key, extent, jnp.float32)
    if cuts:
        array = array * steps_of(key, extent, cuts, -0.22, 0.18)
    return jnp.clip(array, -most, most).astype(kind)


def setup_inputs(seed: int = 0) -> dict:
    seeds = jax.random.split(jax.random.key(seed), 8)
    parcel_props = bell_draw(seeds[0], (PROPS, PARCELS), 1.0, 6.0, ((1, 32),), jnp.float32)
    size_class = place_ends(jax.random.randint(seeds[1], (PARCELS,), 0, CLASSES), jax.random.fold_in(seeds[1], 1), 0, CLASSES - 1).astype(jnp.int32)
    dest_owner_keys = jax.random.split(jax.random.fold_in(seeds[2], 1), PARCELS // PARC_DEV)
    dest_owner_turns = jax.random.permutation(jax.random.fold_in(seeds[2], 3), PARCELS // PARC_DEV)
    dest_owner = jax.vmap(lambda own, number: routed_block(jax.random.fold_in(seeds[2], 2), own, number, PARC_DEV, DEVICES, 1, CAP, 2))(dest_owner_keys, dest_owner_turns).reshape((PARCELS, 1))
    dest_local = place_ends(jax.random.randint(seeds[3], (PARCELS,), 0, LX * LY), jax.random.fold_in(seeds[3], 1), 0, (LX * LY) - 1).astype(jnp.int32)
    class_table = jnp.clip(jnp.exp(jax.random.uniform(seeds[4], (CLASSES, PROPS), jnp.float32, math.log(0.5), math.log(2.0))), 0.5, 2.0)
    gas_density = jnp.clip(jnp.exp(math.log(2.0) - 1.3862944 * jax.random.uniform(seeds[5], (NX, NY), jnp.float32) ** steps_of(seeds[5], (NX, NY), ((0, 8), (1, 4)), -0.2, 0.2)), 0.5, 2.0)
    gas_rest = bell_draw(seeds[6], (4, NX, NY), 1.0, 6.0, ((1, 8), (2, 4)), jnp.float32)
    return dict(parcel_props=parcel_props, size_class=size_class, dest_owner=dest_owner, dest_local=dest_local, class_table=class_table, gas_density=gas_density, gas_rest=gas_rest)


def sources_of(props, classes, gas, table):
    picks = (classes[None, :] == jnp.arange(CLASSES, dtype=jnp.int32)[:, None]).astype(jnp.float32)
    coef = jnp.dot(table.T, picks, precision=lax.Precision.HIGHEST, preferred_element_type=jnp.float32)
    mass = jnp.exp(0.5 * props[0])
    density = gas[0]
    velocity = gas[1:4] / density
    theta = gas[4] / density
    slip = props[1:4] - velocity
    rate = coef[0] * jax.nn.softplus(props[4] - theta)
    evapor = mass * (1.0 - jnp.exp(-rate))
    dragged = 1.0 - jnp.exp(-coef[1] * jnp.sqrt(1.0 + lax.optimization_barrier(jnp.sum(slip * slip, axis=0))))
    moment = evapor * coef[2:5] * props[1:4] + mass * dragged * slip
    energy = evapor * (props[4] + lax.optimization_barrier(jnp.sum(coef[5:] * props[5:], axis=0)))
    return jnp.concatenate([evapor[None], moment, energy[None]], axis=0)

def smooth_field(deposit):
    padded = jnp.pad(deposit, ((0, 0), (1, 1), (1, 1)))
    beside = padded[:, 2:, 1:-1] + padded[:, :-2, 1:-1] + padded[:, 1:-1, 2:] + padded[:, 1:-1, :-2]
    return 0.4 * deposit + 0.15 * beside

def reference(parcel_props, size_class, dest_owner, dest_local, class_table, gas_density, gas_rest):
    owner = dest_owner[:, 0]
    cell_x = owner // N_GY * LX + dest_local // LY
    cell_y = owner % N_GY * LY + dest_local % LY
    flat = (cell_x * NY + cell_y).astype(jnp.int32)
    gas = jnp.concatenate([gas_density[None], gas_rest], axis=0).reshape(5, NX * NY)
    local_gas = gas[:, flat]
    source = sources_of(parcel_props, size_class, local_gas, class_table)
    deposit = jnp.zeros((5, NX * NY), jnp.float32).at[:, flat].add(source).reshape(5, NX, NY)
    smooth = smooth_field(deposit)
    return (gas_density + smooth[0], gas_rest + smooth[1:])
```

```python
import functools

import jax
import jax.numpy as jnp
from jax import lax
from jax.experimental import pallas as pl
from jax.experimental.pallas import tpu as pltpu
from jax.sharding import PartitionSpec as P

F32 = jnp.float32
BF16 = jnp.bfloat16
LANES = 128
ROWS = 8
BATCH = 16
NT = (((1,), (1,)), ((), ()))
MESH = pl.DeviceIdType.MESH


def split(x):
    high = x.astype(BF16).astype(F32)
    return high, x - high


def iota(shape, dim):
    return lax.broadcasted_iota(jnp.int32, shape, dim)


def loop(count, body):
    if count <= 2:
        for step in range(count):
            body(step)
    else:
        lax.fori_loop(0, count, lambda step, unused: (body(step), unused)[1], 0)


def fused_kernel(
    width_x,
    width_y,
    capacity,
    props_hbm,
    class_hbm,
    owner_hbm,
    cell_hbm,
    table_hbm,
    dens_hbm,
    rest_hbm,
    dens_out,
    rest_out,
    props_ref,
    class_ref,
    owner_ref,
    cell_ref,
    table_ref,
    scalars_ref,
    field,
    far_field,
    hot,
    vals,
    keys,
    packed,
    got,
    spot,
    gas,
    tab,
    total,
    far_out,
    far_in,
    row_out,
    row_in,
    col_out,
    col_in,
    load_sem,
    send_sem,
    recv_sem,
    far_send,
    far_recv,
    halo_send,
    halo_recv,
):
    devices = width_x * width_y
    deep = width_x // 2
    team = deep * width_y
    groups = team // ROWS
    my_x, my_y = lax.axis_index("gx"), lax.axis_index("gy")
    half = lax.div(my_x, deep)
    row_of = my_x - half * deep
    me = row_of * width_y + my_y
    base_x = half * deep
    mirror = (row_of + (1 - half) * deep, my_y)
    props_count, parcels = props_ref.shape
    classes = table_ref.shape[0]
    slab_x, slab_y = dens_hbm.shape

    def mate(local):
        return (base_x + lax.div(local, width_y), lax.rem(local, width_y))

    loads = [
        pltpu.make_async_copy(a, b, load_sem.at[i])
        for i, (a, b) in enumerate(
            [
                (owner_hbm, owner_ref),
                (dens_hbm, field.at[0]),
                (rest_hbm, field.at[1:5]),
                (table_hbm, table_ref),
                (class_hbm, class_ref),
                (cell_hbm, cell_ref),
                (props_hbm, props_ref),
                (table_hbm, scalars_ref),
            ]
        )
    ]
    for load in loads:
        load.start()

    barrier = pltpu.get_barrier_semaphore()

    def greet(target):
        pl.semaphore_signal(barrier, inc=1, device_id=target, device_id_type=MESH)

    greet(mirror)
    last_low = (half == 0) & (row_of == deep - 1)
    first_high = (half == 1) & (row_of == 0)

    @pl.when(last_low)
    def _():
        greet((my_x + 1, my_y))

    @pl.when(first_high)
    def _():
        greet((my_x - 1, my_y))

    def greet_mate(k, unused):
        greet(mate(lax.rem(me + k, team)))
        return unused

    lax.fori_loop(1, team, greet_mate, 0, unroll=5 if team == 16 else 1)
    border = jnp.where(last_low | first_high, 1, 0)

    def copy_to(phase, local):
        return pltpu.make_async_remote_copy(
            src_ref=packed.at[phase, local],
            dst_ref=got.at[phase, me],
            send_sem=send_sem.at[phase, local],
            recv_sem=recv_sem.at[phase, me],
            device_id=mate(local),
            device_id_type=MESH,
        )

    def copy_from(phase, local):
        return pltpu.make_async_remote_copy(
            src_ref=packed.at[phase, local],
            dst_ref=got.at[phase, local],
            send_sem=send_sem.at[phase, local],
            recv_sem=recv_sem.at[phase, local],
            device_id=mate(local),
            device_id_type=MESH,
        )

    def far_copy(out_ref, in_ref, i):
        return pltpu.make_async_remote_copy(
            src_ref=out_ref,
            dst_ref=in_ref,
            send_sem=far_send.at[i],
            recv_sem=far_recv.at[i],
            device_id=mirror,
            device_id_type=MESH,
        )

    loads[0].wait()
    row, col = (iota((LANES, 2 * LANES), 0), iota((LANES, 2 * LANES), 1))
    upper = jnp.where((col >= LANES) | (row < col), 1.0, 0.0).astype(BF16)
    ids = iota((devices, LANES), 0)
    wide = hot.shape[0]
    spans = capacity // wide
    ranks = iota((wide, LANES), 0).astype(F32).astype(BF16)
    one, zero = jnp.ones((), BF16), jnp.zeros((), BF16)
    carry = jnp.zeros((devices, LANES), F32)
    chunks = parcels // LANES
    for start in range(0, chunks, ROWS):
        span = range(start, min(start + ROWS, chunks))
        named = [owner_ref[:, c * LANES : (c + 1) * LANES] for c in span]
        mine = [jnp.where(owner == ids, 1.0, 0.0) for owner in named]
        counted = jnp.dot(
            jnp.concatenate(mine, axis=0).astype(BF16), upper, preferred_element_type=F32
        )
        for i, c in enumerate(span):
            part_of = counted[i * devices : (i + 1) * devices]
            rank = jnp.sum(mine[i] * (part_of[:, :LANES] + carry), axis=0, keepdims=True)
            carry = carry + part_of[:, LANES:]
            key = named[i].astype(F32)
            if spans > 1:
                level = sum(jnp.where(rank >= wide * k, 1.0, 0.0) for k in range(1, spans))
                rank = rank - level * wide
                key = key * spans + level
            at = slice(c * LANES, (c + 1) * LANES)
            keys[:, at] = jnp.broadcast_to(key, (2 * ROWS, LANES)).astype(BF16)
            hot[:, at] = jnp.where(ranks == rank.astype(BF16), one, zero)

    for load in loads[1:]:
        load.wait()
    eye = jnp.where(
        iota((props_count, props_count), 0) == iota((props_count, props_count), 1), 1.0, 0.0
    ).astype(BF16)
    table = jnp.concatenate(split(table_ref[...]), axis=0).astype(BF16)
    turned = lax.dot_general(eye, table, NT, preferred_element_type=F32).astype(BF16)
    picks = jnp.where(class_ref[...] == iota((classes, parcels), 0), 1.0, 0.0)
    picks = jnp.concatenate([picks, picks], axis=0).astype(BF16)
    coef = jnp.dot(turned, picks, preferred_element_type=F32)
    props = props_ref[...]
    which = iota((props_count, parcels), 0)
    weights = jnp.where(which >= 5, coef, jnp.where(which == 4, 1.0, 0.0))
    heat_sum = jnp.sum(weights * props, axis=0, keepdims=True)
    which = iota((ROWS, parcels), 0)
    mixed = jnp.where(which == 0, jnp.exp(0.5 * props[0:1]), props[0:ROWS])
    mixed = jnp.where(which == 5, heat_sum, mixed)
    mixed = jnp.where(which == 6, class_ref[...].astype(F32), mixed)
    mixed = jnp.where(which == 7, cell_ref[...].astype(F32), mixed)
    vals[...] = jnp.concatenate(split(mixed), axis=0).astype(BF16)

    pl.semaphore_wait(barrier, team + border)
    far_copy(field, far_field, 0).start()
    batches = team // BATCH

    def send_group(step):
        phase = step // batches
        first = (step % batches) * BATCH
        first_id = jnp.where(phase == half, team, 0) + first
        count = BATCH * spans // 2
        both = [0.0, 0.0]
        for start in range(0, parcels, 256):
            at = slice(start, start + 256)
            for side in range(2):
                sends = [
                    jnp.where(
                        keys[:, at]
                        == (first_id * spans + side * count + i).astype(F32).astype(BF16),
                        vals[:, at],
                        zero,
                    )
                    for i in range(count)
                ]
                both[side] += lax.dot_general(
                    jnp.concatenate(sends, axis=0),
                    hot[:, at],
                    NT,
                    preferred_element_type=F32,
                )
        both = jnp.concatenate(both, axis=0)
        for i in range(BATCH):
            for k in range(spans):
                at = 2 * ROWS * (i * spans + k)
                packed[phase, first + i, :, k * wide : (k + 1) * wide] = (
                    both[at : at + ROWS] + both[at + ROWS : at + 2 * ROWS]
                )

        def launch(i, carried):
            local = first + lax.rem(me + i, BATCH)

            @pl.when(local != me)
            def _():
                copy_to(phase, local).start()

            return carried

        lax.fori_loop(1, BATCH + 1, launch, 0, unroll=True)

    loop(2 * batches, send_group)
    for phase in range(2):
        got[phase, me] = packed[phase, me]

    half_x = slab_x // 2
    ys = iota((2 * slab_y, capacity), 0).astype(F32).astype(BF16)
    xs = iota((half_x, capacity), 0)
    xs_short = xs.astype(F32).astype(BF16)

    def run_phase(phase, fields):
        parts = []
        for c in range(5):
            for piece in split(fields[c]):
                parts.append(jnp.concatenate([piece[:half_x], piece[half_x:]], axis=1))
        tab[...] = jnp.concatenate(parts, axis=0).astype(BF16)
        total[...] = jnp.zeros_like(total)

        def take_group(step, unused):
            turn = lax.div(me, ROWS) + step
            first = lax.rem(turn, groups) * ROWS

            def arrive(i, carried):
                @pl.when(first + i != me)
                def _():
                    copy_from(phase, first + i).wait_recv()

                return carried

            lax.fori_loop(0, ROWS, arrive, 0, unroll=True)

            def part(c):
                return jnp.concatenate(
                    [got[phase, first + i][c : c + 1] for i in range(ROWS)], axis=0
                )

            cell = part(7).astype(jnp.int32)
            line = lax.div(cell, slab_y)
            upper_half = jnp.where(line >= half_x, 1, 0)
            lanes_at = (cell - line * slab_y + upper_half * slab_y).astype(F32)
            lines_at = line - upper_half * half_x
            lines_short = lines_at.astype(F32)
            for i in range(ROWS):
                spot_at = slice(i * capacity, (i + 1) * capacity)
                spot[:, spot_at] = jnp.where(
                    ys == lanes_at[i : i + 1].astype(BF16), one, zero
                )
                found = jnp.dot(tab[...], spot[:, spot_at], preferred_element_type=F32)
                in_row = xs == lines_at[i : i + 1]
                for c in range(5):
                    at = 2 * c * half_x
                    both = found[at : at + half_x] + found[at + half_x : at + 2 * half_x]
                    gas[c, i : i + 1] = jnp.sum(
                        jnp.where(in_row, both, 0.0), axis=0, keepdims=True
                    )

            kind = part(6).astype(jnp.int32)
            coefs = [jnp.full(kind.shape, scalars_ref[0, j], F32) for j in range(5)]
            for k in range(1, classes):
                same = kind == k
                coefs = [jnp.where(same, scalars_ref[k, j], coefs[j]) for j in range(5)]
            mass = part(0)
            speed = [part(j) for j in (1, 2, 3)]
            heat, energy = part(4), part(5)
            inverse = 1.0 / gas[0]
            slip = [speed[j] - gas[j + 1] * inverse for j in range(3)]
            excess = heat - gas[4] * inverse
            soft = jnp.maximum(excess, 0.0) + jnp.log1p(jnp.exp(-jnp.abs(excess)))
            evapor = mass * (1.0 - jnp.exp(-(coefs[0] * soft)))
            square = slip[0] * slip[0] + slip[1] * slip[1] + slip[2] * slip[2]
            drag = mass * (1.0 - jnp.exp(-coefs[1] * jnp.sqrt(1.0 + square)))
            out = [evapor]
            out += [evapor * coefs[2 + j] * speed[j] + drag * slip[j] for j in range(3)]
            out += [evapor * energy]

            pieces = [piece for c in range(5) for piece in split(out[c])]
            spread = []
            for i in range(ROWS):
                in_row = xs_short == lines_short[i : i + 1].astype(BF16)
                spread.append(
                    jnp.concatenate(
                        [
                            jnp.where(in_row, piece[i : i + 1].astype(BF16), zero)
                            for piece in pieces
                        ],
                        axis=0,
                    )
                )
            part_total = 0.0
            for at in (0, ROWS // 2):
                part_total += lax.dot_general(
                    jnp.concatenate(spread[at : at + ROWS // 2], axis=1),
                    spot[:, at * capacity : (at + ROWS // 2) * capacity],
                    NT,
                    preferred_element_type=F32,
                )
            total[...] += part_total
            return unused

        lax.fori_loop(0, groups, take_group, 0)
        summed = []
        for c in range(5):
            at = 2 * c * half_x
            both = total[at : at + half_x] + total[at + half_x : at + 2 * half_x]
            summed.append(jnp.concatenate([both[:, :slab_y], both[:, slab_y:]], axis=0))
        return summed

    far_copy(field, far_field, 0).wait_recv()
    for c, piece in enumerate(run_phase(0, far_field)):
        far_out[c] = piece
    far_copy(far_out, far_in, 1).start()
    mine = run_phase(1, field)
    far_copy(far_out, far_in, 1).wait_recv()
    deposit = [mine[c] + far_in[c] for c in range(5)]
    lane = iota((slab_x, slab_y), 1)
    low_edge = jnp.zeros((slab_x, slab_y), F32)
    high_edge = jnp.zeros((slab_x, slab_y), F32)
    row_out[...] = jnp.zeros_like(row_out)
    for c in range(5):
        row_out[0, c : c + 1] = deposit[c][0:1]
        row_out[1, c : c + 1] = deposit[c][slab_x - 1 : slab_x]
        low_edge = jnp.where(
            lane == c, pltpu.roll(deposit[c], c, 1) if c else deposit[c], low_edge
        )
        high_edge = jnp.where(lane == c, pltpu.roll(deposit[c], c + 1, 1), high_edge)
    col_out[0] = low_edge
    col_out[1] = high_edge

    def edge(out_ref, in_ref, side, base, target):
        return pltpu.make_async_remote_copy(
            src_ref=out_ref.at[side],
            dst_ref=in_ref.at[side],
            send_sem=halo_send.at[base + side],
            recv_sem=halo_recv.at[base + side],
            device_id=target,
            device_id_type=MESH,
        )

    edges = [
        (row_out, row_in, 0, 0, (my_x - 1, my_y), my_x > 0, my_x < width_x - 1),
        (row_out, row_in, 1, 0, (my_x + 1, my_y), my_x < width_x - 1, my_x > 0),
        (col_out, col_in, 0, 2, (my_x, my_y - 1), my_y > 0, my_y < width_y - 1),
        (col_out, col_in, 1, 2, (my_x, my_y + 1), my_y < width_y - 1, my_y > 0),
    ]
    for out_ref, in_ref, side, base, target, sends, takes in edges:

        @pl.when(sends)
        def _(out_ref=out_ref, in_ref=in_ref, side=side, base=base, target=target):
            edge(out_ref, in_ref, side, base, target).start()

        @pl.when(jnp.logical_not(takes))
        def _(in_ref=in_ref, side=side):
            in_ref[side] = jnp.zeros(in_ref.shape[1:], F32)

    def wait_sent(k, unused):
        local = lax.rem(me + k, team)
        for phase in range(2):
            copy_to(phase, local).wait_send()
        return unused

    lax.fori_loop(1, team, wait_sent, 0)
    far_copy(field, far_field, 0).wait_send()
    far_copy(far_out, far_in, 1).wait_send()
    for out_ref, in_ref, side, base, target, sends, takes in edges:

        @pl.when(takes)
        def _(out_ref=out_ref, in_ref=in_ref, side=side, base=base, target=target):
            edge(out_ref, in_ref, side, base, target).wait_recv()

    for c in range(5):
        here = deposit[c]
        above = jnp.concatenate([row_in[1, c : c + 1], here[: slab_x - 1]], axis=0)
        below = jnp.concatenate([here[1:], row_in[0, c : c + 1]], axis=0)
        left_in = pltpu.roll(col_in[1], slab_y - c, 1) if c else col_in[1]
        left = jnp.where(lane == 0, left_in, pltpu.roll(here, 1, 1))
        right = jnp.where(
            lane == slab_y - 1,
            pltpu.roll(col_in[0], slab_y - 1 - c, 1),
            pltpu.roll(here, slab_y - 1, 1),
        )
        smooth = 0.4 * here + 0.15 * (below + above + right + left)
        if c:
            rest_out[c - 1] = field[c] + smooth
        else:
            dens_out[...] = field[0] + smooth

    for out_ref, in_ref, side, base, target, sends, takes in edges:

        @pl.when(sends)
        def _(out_ref=out_ref, in_ref=in_ref, side=side, base=base, target=target):
            edge(out_ref, in_ref, side, base, target).wait_send()


def per_device(
    parcel_props, size_class, dest_owner, dest_local, class_table, gas_density, gas_rest
):
    width_x, width_y = lax.axis_size("gx"), lax.axis_size("gy")
    devices = width_x * width_y
    team = devices // 2
    props_count, parcels = parcel_props.shape
    slab_x, slab_y = gas_density.shape
    capacity = -(-max(2, 4 * parcels // devices) // LANES) * LANES
    hbm = pl.BlockSpec(memory_space=pl.ANY)
    vmem = pl.BlockSpec(memory_space=pltpu.VMEM)
    dens, rest = pl.pallas_call(
        functools.partial(fused_kernel, width_x, width_y, capacity),
        out_shape=(
            pltpu.VMEM((slab_x, slab_y), F32),
            pltpu.VMEM((4, slab_x, slab_y), F32),
        ),
        in_specs=[hbm] * 7,
        out_specs=(vmem, vmem),
        scratch_shapes=[
            pltpu.VMEM((props_count, parcels), F32),
            pltpu.VMEM((1, parcels), jnp.int32),
            pltpu.VMEM((1, parcels), jnp.int32),
            pltpu.VMEM((1, parcels), jnp.int32),
            pltpu.VMEM(class_table.shape, F32),
            pltpu.SMEM(class_table.shape, F32),
            pltpu.VMEM((5, slab_x, slab_y), F32),
            pltpu.VMEM((5, slab_x, slab_y), F32),
            pltpu.VMEM((min(capacity, 256), parcels), BF16),
            pltpu.VMEM((2 * ROWS, parcels), BF16),
            pltpu.VMEM((2 * ROWS, parcels), BF16),
            pltpu.VMEM((2, team, ROWS, capacity), F32),
            pltpu.VMEM((2, team, ROWS, capacity), F32),
            pltpu.VMEM((2 * slab_y, ROWS * capacity), BF16),
            pltpu.VMEM((5, ROWS, capacity), F32),
            pltpu.VMEM((5 * slab_x, 2 * slab_y), BF16),
            pltpu.VMEM((5 * slab_x, 2 * slab_y), F32),
            pltpu.VMEM((5, slab_x, slab_y), F32),
            pltpu.VMEM((5, slab_x, slab_y), F32),
            pltpu.VMEM((2, ROWS, slab_y), F32),
            pltpu.VMEM((2, ROWS, slab_y), F32),
            pltpu.VMEM((2, slab_x, slab_y), F32),
            pltpu.VMEM((2, slab_x, slab_y), F32),
            pltpu.SemaphoreType.DMA((8,)),
            pltpu.SemaphoreType.DMA((2, team)),
            pltpu.SemaphoreType.DMA((2, team)),
            pltpu.SemaphoreType.DMA((2,)),
            pltpu.SemaphoreType.DMA((2,)),
            pltpu.SemaphoreType.DMA((4,)),
            pltpu.SemaphoreType.DMA((4,)),
        ],
        compiler_params=pltpu.CompilerParams(collective_id=0, has_side_effects=True),
    )(
        parcel_props,
        size_class.reshape(1, parcels),
        dest_owner.reshape(1, parcels),
        dest_local.reshape(1, parcels),
        class_table,
        gas_density,
        gas_rest,
    )
    return pl.pallas_call(
        store_kernel,
        out_shape=(
            jax.ShapeDtypeStruct(dens.shape, F32),
            jax.ShapeDtypeStruct(rest.shape, F32),
        ),
        in_specs=[hbm, hbm],
        out_specs=(hbm, hbm),
        scratch_shapes=[pltpu.SemaphoreType.DMA((2,))],
    )(*(pltpu.with_memory_space_constraint(x, pltpu.VMEM) for x in (dens, rest)))


def store_kernel(dens_ref, rest_ref, dens_out, rest_out, sem):
    stores = [
        pltpu.make_async_copy(dens_ref, dens_out, sem.at[0]),
        pltpu.make_async_copy(rest_ref, rest_out, sem.at[1]),
    ]
    for store in stores:
        store.start()
    for store in stores:
        store.wait()


def solution(mesh):
    return jax.shard_map(
        per_device,
        mesh=mesh,
        in_specs=(
            P(None, ("gx", "gy")),
            P(("gx", "gy")),
            P(("gx", "gy"), None),
            P(("gx", "gy")),
            P(),
            P("gx", "gy"),
            P(None, "gx", "gy"),
        ),
        out_specs=(P("gx", "gy"), P(None, "gx", "gy")),
        check_vma=False,
    )
```

```python
import functools

import jax
import jax.numpy as jnp
from jax import lax
from jax.experimental import pallas as pl
from jax.experimental.pallas import tpu as pltpu
from jax.sharding import PartitionSpec as P

F32 = jnp.float32
BF16 = jnp.bfloat16
F8 = jnp.float8_e4m3fn
LANES = 128
ROWS = 8
NT = (((1,), (1,)), ((), ()))
MESH = pl.DeviceIdType.MESH


def split(x):
    high = x.astype(BF16).astype(F32)
    return high, x - high


def pick(table, index, axis):
    other = (1 - axis,)
    return lax.gather(
        table,
        index[..., None],
        lax.GatherDimensionNumbers(
            offset_dims=(),
            collapsed_slice_dims=(axis,),
            start_index_map=(axis,),
            operand_batching_dims=other,
            start_indices_batching_dims=other,
        ),
        slice_sizes=(1, 1),
        mode=lax.GatherScatterMode.PROMISE_IN_BOUNDS,
    )


def iota(shape, dim):
    return lax.broadcasted_iota(jnp.int32, shape, dim)


def fused_kernel(
    width_x,
    width_y,
    capacity,
    props_hbm,
    class_hbm,
    owner_hbm,
    cell_hbm,
    table_hbm,
    dens_hbm,
    rest_hbm,
    dens_out,
    rest_out,
    props_ref,
    class_ref,
    owner_ref,
    cell_ref,
    table_ref,
    scalars_ref,
    field,
    far_field,
    hot,
    vals,
    keys,
    packed,
    got,
    spot,
    tab,
    total,
    far_out,
    far_in,
    row_out,
    row_in,
    col_out,
    col_in,
    load_sem,
    send_sem,
    recv_sem,
    far_send,
    far_recv,
    halo_send,
    halo_recv,
):
    devices = width_x * width_y
    deep = width_x // 2
    team = deep * width_y
    groups = team // ROWS
    tiles = capacity // LANES
    block = tiles * ROWS
    my_x, my_y = lax.axis_index("gx"), lax.axis_index("gy")
    half = lax.div(my_x, deep)
    row_of = my_x - half * deep
    me = row_of * width_y + my_y
    base_x = half * deep
    mirror = (row_of + (1 - half) * deep, my_y)
    props_count, parcels = props_ref.shape
    classes = table_ref.shape[0]
    slab_x, slab_y = dens_hbm.shape

    def mate(local):
        return (base_x + lax.div(local, width_y), lax.rem(local, width_y))

    loads = [
        pltpu.make_async_copy(a, b, load_sem.at[i])
        for i, (a, b) in enumerate(
            [
                (owner_hbm, owner_ref),
                (dens_hbm, field.at[0]),
                (rest_hbm, field.at[1:5]),
                (table_hbm, table_ref),
                (class_hbm, class_ref),
                (cell_hbm, cell_ref),
                (props_hbm, props_ref),
                (table_hbm, scalars_ref),
            ]
        )
    ]
    for load in loads:
        load.start()

    barrier = pltpu.get_barrier_semaphore()

    def greet(target):
        pl.semaphore_signal(barrier, inc=1, device_id=target, device_id_type=MESH)

    def greet_mate(k, unused):
        greet(mate(lax.rem(me + k, team)))
        return unused

    middle = team // 2
    lax.fori_loop(middle, team, greet_mate, 0, unroll=True if team == 16 else 1)
    greet(mirror)
    last_low = (half == 0) & (row_of == deep - 1)
    first_high = (half == 1) & (row_of == 0)

    @pl.when(last_low)
    def _():
        greet((my_x + 1, my_y))

    @pl.when(first_high)
    def _():
        greet((my_x - 1, my_y))

    around = [
        ((mirror[0] + 1, my_y), row_of < deep - 1),
        ((mirror[0] - 1, my_y), row_of > 0),
        ((mirror[0], my_y + 1), my_y < width_y - 1),
        ((mirror[0], my_y - 1), my_y > 0),
    ]
    greets = team + jnp.where(last_low | first_high, 1, 0)
    for target, there in around:
        greets = greets + jnp.where(there, 1, 0)

        @pl.when(there)
        def _():
            greet(target)

    lax.fori_loop(1, middle, greet_mate, 0, unroll=True if team == 16 else 1)

    def rows_of(local):
        return pl.ds(pl.multiple_of(local * block, ROWS), block)

    def copy_to(phase, local):
        return pltpu.make_async_remote_copy(
            src_ref=packed.at[phase, local],
            dst_ref=got.at[phase, rows_of(me)],
            send_sem=send_sem.at[phase, local],
            recv_sem=recv_sem.at[phase, me],
            device_id=mate(local),
            device_id_type=MESH,
        )

    def copy_from(phase, local):
        return pltpu.make_async_remote_copy(
            src_ref=packed.at[phase, local],
            dst_ref=got.at[phase, rows_of(local)],
            send_sem=send_sem.at[phase, local],
            recv_sem=recv_sem.at[phase, local],
            device_id=mate(local),
            device_id_type=MESH,
        )

    def far_copy(out_ref, in_ref, i):
        return pltpu.make_async_remote_copy(
            src_ref=out_ref,
            dst_ref=in_ref,
            send_sem=far_send.at[i],
            recv_sem=far_recv.at[i],
            device_id=mirror,
            device_id_type=MESH,
        )

    loads[0].wait()
    row, col = (iota((LANES, 2 * LANES), 0), iota((LANES, 2 * LANES), 1))
    upper = jnp.where((col >= LANES) | (row < col), 1.0, 0.0).astype(BF16)
    ids = iota((devices, LANES), 0)
    wide = hot.shape[0]
    spans = capacity // wide
    ranks = iota((wide, LANES), 0).astype(F32).astype(BF16)
    one, zero = jnp.ones((), BF16), jnp.zeros((), BF16)
    carry = jnp.zeros((devices, LANES), F32)
    chunks = parcels // LANES
    for start in range(0, chunks, ROWS):
        span = range(start, min(start + ROWS, chunks))
        named = [owner_ref[:, c * LANES : (c + 1) * LANES] for c in span]
        mine = [jnp.where(owner == ids, 1.0, 0.0) for owner in named]
        counted = jnp.dot(
            jnp.concatenate(mine, axis=0).astype(BF16), upper, preferred_element_type=F32
        )
        for i, c in enumerate(span):
            part_of = counted[i * devices : (i + 1) * devices]
            rank = jnp.sum(mine[i] * (part_of[:, :LANES] + carry), axis=0, keepdims=True)
            carry = carry + part_of[:, LANES:]
            key = named[i].astype(F32)
            if spans > 1:
                level = sum(jnp.where(rank >= wide * k, 1.0, 0.0) for k in range(1, spans))
                rank = rank - level * wide
                key = key * spans + level
            at = slice(c * LANES, (c + 1) * LANES)
            keys[:, at] = jnp.broadcast_to(key, (2 * ROWS, LANES)).astype(BF16)
            hot[:, at] = jnp.where(ranks == rank.astype(BF16), one, zero).astype(F8)

    for load in loads[1:]:
        load.wait()
    eye = jnp.where(
        iota((props_count, props_count), 0) == iota((props_count, props_count), 1), 1.0, 0.0
    ).astype(BF16)
    table = jnp.concatenate(split(table_ref[...]), axis=0).astype(BF16)
    turned = lax.dot_general(eye, table, NT, preferred_element_type=F32).astype(BF16)
    picks = jnp.where(class_ref[...] == iota((classes, parcels), 0), 1.0, 0.0)
    picks = jnp.concatenate([picks, picks], axis=0).astype(BF16)
    coef = jnp.dot(turned, picks, preferred_element_type=F32)
    props = props_ref[...]
    which = iota((props_count, parcels), 0)
    weights = jnp.where(which >= 5, coef, jnp.where(which == 4, 1.0, 0.0))
    heat_sum = jnp.sum(weights * props, axis=0, keepdims=True)
    which = iota((ROWS, parcels), 0)
    mixed = jnp.where(which == 0, jnp.exp(0.5 * props[0:1]), props[0:ROWS])
    mixed = jnp.where(which == 5, heat_sum, mixed)
    mixed = jnp.where(which == 6, class_ref[...].astype(F32), mixed)
    mixed = jnp.where(which == 7, cell_ref[...].astype(F32), mixed)
    vals[...] = jnp.concatenate(split(mixed), axis=0).astype(BF16)

    def first_of(turn):
        return lax.rem(lax.div(me, ROWS) + turn, groups) * ROWS

    def pack(phase, turn):
        first = first_of(turn)
        first_id = (half * team if phase else (1 - half) * team) + first
        count = ROWS * spans // 2
        both = [0.0, 0.0]
        for start in range(0, parcels, 256):
            at = slice(start, start + 256)
            for side in range(2):
                sends = [
                    jnp.where(
                        keys[:, at]
                        == (first_id * spans + side * count + i).astype(F32).astype(BF16),
                        vals[:, at],
                        zero,
                    )
                    for i in range(count)
                ]
                both[side] += lax.dot_general(
                    jnp.concatenate(sends, axis=0),
                    hot[:, at],
                    NT,
                    preferred_element_type=F32,
                )
        both = jnp.concatenate(both, axis=0)
        for i in range(ROWS):
            for k in range(spans):
                at = 2 * ROWS * (i * spans + k)
                whole = both[at : at + ROWS] + both[at + ROWS : at + 2 * ROWS]
                for t in range(wide // LANES):
                    tile = k * (wide // LANES) + t
                    packed[phase, first + i, tile * ROWS : (tile + 1) * ROWS] = whole[
                        :, t * LANES : (t + 1) * LANES
                    ]

    def launch(phase, turn, near):
        for i in range(1, ROWS if near else ROWS + 1):
            copy_to(phase, first_of(turn) + lax.rem(me + i, ROWS)).start()

    def send(phase, turn, near):
        pack(phase, turn)
        launch(phase, turn, near)

    def send_others(phase, start):
        if groups - start <= 2:
            for turn in range(start, groups):
                send(phase, turn, False)
        else:
            lax.fori_loop(start, groups, lambda k, u: (send(phase, k, False), u)[1], 0)

    early = row_of * 2 < deep
    pack(0, 0)
    if groups > 1:
        pack(0, 1)
    pl.semaphore_wait(barrier, greets)

    @pl.when(early)
    def _():
        far_copy(field, far_field, 0).start()

    launch(0, 0, True)
    if groups > 1:
        launch(0, 1, False)
        send_others(0, 2)

    @pl.when(jnp.logical_not(early))
    def _():
        far_copy(field, far_field, 0).start()

    send(1, 0, True)
    send_others(1, 1)
    for phase in range(2):
        got[phase, rows_of(me)] = packed[phase, me]

    half_x = slab_x // 2
    ys = iota((2 * slab_y, capacity), 0).astype(F32).astype(BF16)
    xs_short = iota((half_x, capacity), 0).astype(F32).astype(BF16)
    sub = iota((ROWS, LANES), 0)

    def prepare(phase, fields):
        parts = []
        for c in range(5):
            for piece in split(fields[c]):
                parts.append(jnp.concatenate([piece[:half_x], piece[half_x:]], axis=1))
        tab[phase] = jnp.concatenate(parts, axis=0).astype(BF16)

    def take_group(phase, turn):
        if True:
            first = first_of(turn)

            def arrive(i, carried):
                @pl.when(first + i != me)
                def _():
                    copy_from(phase, first + i).wait_recv()

                return carried

            lax.fori_loop(0, ROWS, arrive, 0, unroll=True)

            def part(c):
                return jnp.concatenate(
                    [
                        got[phase, pl.ds(first * block + t * ROWS + c, ROWS, stride=block), :]
                        for t in range(tiles)
                    ],
                    axis=1,
                )

            cell = part(7).astype(jnp.int32)
            line = lax.div(cell, slab_y)
            lane_of = cell - line * slab_y
            upper_half = jnp.where(line >= half_x, 1, 0)
            lanes_at = (lane_of + upper_half * slab_y).astype(F32)
            lines_short = (line - upper_half * half_x).astype(F32)
            line_at = line - upper_half * half_x
            shelf = lax.div(line_at, ROWS)
            within = line_at - shelf * ROWS
            gas = [[jnp.zeros((ROWS, LANES), F32)] * tiles for c in range(5)]
            for i in range(ROWS):
                spot_at = slice(i * capacity, (i + 1) * capacity)
                spot[:, spot_at] = jnp.where(
                    ys == lanes_at[i : i + 1].astype(BF16), one, zero
                ).astype(F8)
                found = jnp.dot(tab[phase], spot[:, spot_at], preferred_element_type=F32)
                for t in range(tiles):
                    lanes = slice(t * LANES, (t + 1) * LANES)
                    low, deep_row = [
                        jnp.broadcast_to(x[i : i + 1, lanes], (ROWS, LANES))
                        for x in (within, shelf)
                    ]
                    for c in range(5):
                        pieces = []
                        for p in range(2):
                            at = (2 * c + p) * half_x
                            piece = found[at : at + ROWS, lanes]
                            for r in range(1, half_x // ROWS):
                                here = found[at + r * ROWS : at + (r + 1) * ROWS, lanes]
                                piece = jnp.where(deep_row >= r, here, piece)
                            pieces.append(piece)
                        gas[c][t] = jnp.where(
                            sub == i, pick(pieces[0] + pieces[1], low, 0), gas[c][t]
                        )
            gas = [jnp.concatenate(row, axis=1) for row in gas]

            kind = part(6).astype(jnp.int32)
            coefs = [jnp.full(kind.shape, scalars_ref[0, j], F32) for j in range(5)]
            for k in range(1, classes):
                same = kind == k
                coefs = [jnp.where(same, scalars_ref[k, j], coefs[j]) for j in range(5)]
            mass = part(0)
            speed = [part(j) for j in (1, 2, 3)]
            heat, energy = part(4), part(5)
            inverse = 1.0 / gas[0]
            slip = [speed[j] - gas[j + 1] * inverse for j in range(3)]
            excess = heat - gas[4] * inverse
            soft = jnp.maximum(excess, 0.0) + jnp.log1p(jnp.exp(-jnp.abs(excess)))
            evapor = mass * (1.0 - jnp.exp(-(coefs[0] * soft)))
            square = slip[0] * slip[0] + slip[1] * slip[1] + slip[2] * slip[2]
            drag = mass * (1.0 - jnp.exp(-coefs[1] * jnp.sqrt(1.0 + square)))
            out = [evapor]
            out += [evapor * coefs[2 + j] * speed[j] + drag * slip[j] for j in range(3)]
            out += [evapor * energy]

            pieces = [piece for c in range(5) for piece in split(out[c])]
            spread = []
            for i in range(ROWS):
                in_row = xs_short == lines_short[i : i + 1].astype(BF16)
                spread.append(
                    jnp.concatenate(
                        [
                            jnp.where(in_row, piece[i : i + 1].astype(BF16), zero)
                            for piece in pieces
                        ],
                        axis=0,
                    )
                )
            for side in range(2):
                at = side * ROWS // 2
                total[phase, side] += lax.dot_general(
                    jnp.concatenate(spread[at : at + ROWS // 2], axis=1),
                    spot[:, at * capacity : (at + ROWS // 2) * capacity],
                    NT,
                    preferred_element_type=F32,
                )

    def deposit_of(phase):
        whole = total[phase, 0] + total[phase, 1]
        summed = []
        for c in range(5):
            at = 2 * c * half_x
            both = whole[at : at + half_x] + whole[at + half_x : at + 2 * half_x]
            summed.append(jnp.concatenate([both[:, :slab_y], both[:, slab_y:]], axis=0))
        return summed

    lane = iota((slab_x, slab_y), 1)

    def edges_of(origin):
        x, y = origin
        return [
            (row_out, row_in, 0, 0, (x - 1, y), x > 0, my_x < width_x - 1),
            (row_out, row_in, 1, 0, (x + 1, y), x < width_x - 1, my_x > 0),
            (col_out, col_in, 0, 2, (x, y - 1), y > 0, my_y < width_y - 1),
            (col_out, col_in, 1, 2, (x, y + 1), y < width_y - 1, my_y > 0),
        ]

    def edge(phase, out_ref, in_ref, side, base, target):
        at = 4 * phase + base + side
        return pltpu.make_async_remote_copy(
            src_ref=out_ref.at[phase, side],
            dst_ref=in_ref.at[phase, side],
            send_sem=halo_send.at[at],
            recv_sem=halo_recv.at[at],
            device_id=target,
            device_id_type=MESH,
        )

    origins = (mirror, (my_x, my_y))

    def send_edges(phase, deposit):
        sides = jnp.zeros((slab_x, slab_y), F32)
        for c in range(5):
            row_out[phase, 0, c : c + 1] = deposit[c][0:1]
            row_out[phase, 1, c : c + 1] = deposit[c][slab_x - 1 : slab_x]
            first = pltpu.roll(deposit[c], c, 1) if c else deposit[c]
            sides = jnp.where(lane == c, first, sides)
            last = pltpu.roll(deposit[c], ROWS + c + 1, 1)
            sides = jnp.where(lane == ROWS + c, last, sides)
        turned = jnp.transpose(sides)
        for side in range(2):
            col_out[phase, side, :, :slab_x] = turned[side * ROWS : (side + 1) * ROWS]
        for out_ref, in_ref, side, base, target, sends, takes in edges_of(origins[phase]):

            @pl.when(sends)
            def _():
                edge(phase, out_ref, in_ref, side, base, target).start()

    for ref in (row_out, col_out):
        ref[...] = jnp.zeros_like(ref)
    for out_ref, in_ref, side, base, target, sends, takes in edges_of(origins[1]):

        @pl.when(jnp.logical_not(takes))
        def _():
            for phase in range(2):
                in_ref[phase, side] = jnp.zeros(in_ref.shape[2:], F32)

    total[...] = jnp.zeros_like(total)
    prepare(1, field)
    lead = jnp.where(early, 0, 1)

    def step(t, unused):
        at = t - lead

        @pl.when(at == 0)
        def _():
            far_copy(field, far_field, 0).wait_recv()
            prepare(0, far_field)

        far_turn = (at >= 0) & (at < groups)
        phase = jnp.where(far_turn, 0, 1)
        take_group(phase, jnp.where(far_turn, at, jnp.where(at < 0, 0, t - groups)))

        @pl.when(at == groups - 1)
        def _():
            deposit = deposit_of(0)
            for c in range(5):
                far_out[c] = deposit[c]
            send_edges(0, deposit)
            far_copy(far_out, far_in, 1).start()

        return unused

    lax.fori_loop(0, 2 * groups, step, 0)
    mine = deposit_of(1)
    send_edges(1, mine)
    def wait_sent(k, unused):
        local = lax.rem(me + k, team)
        for phase in range(2):
            copy_to(phase, local).wait_send()
        return unused

    lax.fori_loop(1, team, wait_sent, 0)
    far_copy(field, far_field, 0).wait_send()
    far_copy(far_out, far_in, 1).wait_send()
    far_copy(far_out, far_in, 1).wait_recv()
    for phase in range(2):
        for out_ref, in_ref, side, base, target, sends, takes in edges_of(origins[1]):

            @pl.when(takes)
            def _():
                edge(phase, out_ref, in_ref, side, base, target).wait_recv()

    rows_in = [row_in[0, side] + row_in[1, side] for side in range(2)]
    cols_in = [
        jnp.transpose(col_in[0, side] + col_in[1, side])[:slab_x] for side in range(2)
    ]
    for c in range(5):
        here = mine[c] + far_in[c]
        above = jnp.concatenate([rows_in[1][c : c + 1], here[: slab_x - 1]], axis=0)
        below = jnp.concatenate([here[1:], rows_in[0][c : c + 1]], axis=0)
        beside = [jnp.broadcast_to(x[:, c : c + 1], (slab_x, slab_y)) for x in cols_in]
        left = jnp.where(lane == 0, beside[1], pltpu.roll(here, 1, 1))
        right = jnp.where(lane == slab_y - 1, beside[0], pltpu.roll(here, slab_y - 1, 1))
        smooth = 0.4 * here + 0.15 * (below + above + right + left)
        if c:
            rest_out[c - 1] = field[c] + smooth
        else:
            dens_out[...] = field[0] + smooth

    for phase in range(2):
        for out_ref, in_ref, side, base, target, sends, takes in edges_of(origins[phase]):

            @pl.when(sends)
            def _():
                edge(phase, out_ref, in_ref, side, base, target).wait_send()


def per_device(
    parcel_props, size_class, dest_owner, dest_local, class_table, gas_density, gas_rest
):
    width_x, width_y = lax.axis_size("gx"), lax.axis_size("gy")
    devices = width_x * width_y
    team = devices // 2
    props_count, parcels = parcel_props.shape
    slab_x, slab_y = gas_density.shape
    capacity = -(-max(2, 4 * parcels // devices) // LANES) * LANES
    hbm = pl.BlockSpec(memory_space=pl.ANY)
    vmem = pl.BlockSpec(memory_space=pltpu.VMEM)
    dens, rest = pl.pallas_call(
        functools.partial(fused_kernel, width_x, width_y, capacity),
        out_shape=(
            pltpu.VMEM((slab_x, slab_y), F32),
            pltpu.VMEM((4, slab_x, slab_y), F32),
        ),
        in_specs=[hbm] * 7,
        out_specs=(vmem, vmem),
        scratch_shapes=[
            pltpu.VMEM((props_count, parcels), F32),
            pltpu.VMEM((1, parcels), jnp.int32),
            pltpu.VMEM((1, parcels), jnp.int32),
            pltpu.VMEM((1, parcels), jnp.int32),
            pltpu.VMEM(class_table.shape, F32),
            pltpu.SMEM(class_table.shape, F32),
            pltpu.VMEM((5, slab_x, slab_y), F32),
            pltpu.VMEM((5, slab_x, slab_y), F32),
            pltpu.VMEM((min(capacity, 256), parcels), F8),
            pltpu.VMEM((2 * ROWS, parcels), BF16),
            pltpu.VMEM((2 * ROWS, parcels), BF16),
            pltpu.VMEM((2, team, capacity // LANES * ROWS, LANES), F32),
            pltpu.VMEM((2, team * capacity // LANES * ROWS, LANES), F32),
            pltpu.VMEM((2 * slab_y, ROWS * capacity), F8),
            pltpu.VMEM((2, 5 * slab_x, 2 * slab_y), BF16),
            pltpu.VMEM((2, 2, 5 * slab_x, 2 * slab_y), F32),
            pltpu.VMEM((5, slab_x, slab_y), F32),
            pltpu.VMEM((5, slab_x, slab_y), F32),
            pltpu.VMEM((2, 2, ROWS, slab_y), F32),
            pltpu.VMEM((2, 2, ROWS, slab_y), F32),
            pltpu.VMEM((2, 2, ROWS, LANES), F32),
            pltpu.VMEM((2, 2, ROWS, LANES), F32),
            pltpu.SemaphoreType.DMA((8,)),
            pltpu.SemaphoreType.DMA((2, team)),
            pltpu.SemaphoreType.DMA((2, team)),
            pltpu.SemaphoreType.DMA((2,)),
            pltpu.SemaphoreType.DMA((2,)),
            pltpu.SemaphoreType.DMA((8,)),
            pltpu.SemaphoreType.DMA((8,)),
        ],
        compiler_params=pltpu.CompilerParams(collective_id=0, has_side_effects=True),
    )(
        parcel_props,
        size_class.reshape(1, parcels),
        dest_owner.reshape(1, parcels),
        dest_local.reshape(1, parcels),
        class_table,
        gas_density,
        gas_rest,
    )
    return pl.pallas_call(
        store_kernel,
        out_shape=(
            jax.ShapeDtypeStruct(dens.shape, F32),
            jax.ShapeDtypeStruct(rest.shape, F32),
        ),
        in_specs=[hbm, hbm],
        out_specs=(hbm, hbm),
        scratch_shapes=[pltpu.SemaphoreType.DMA((2,))],
    )(*(pltpu.with_memory_space_constraint(x, pltpu.VMEM) for x in (dens, rest)))


def store_kernel(dens_ref, rest_ref, dens_out, rest_out, sem):
    stores = [
        pltpu.make_async_copy(dens_ref, dens_out, sem.at[0]),
        pltpu.make_async_copy(rest_ref, rest_out, sem.at[1]),
    ]
    for store in stores:
        store.start()
    for store in stores:
        store.wait()


def solution(mesh):
    return jax.shard_map(
        per_device,
        mesh=mesh,
        in_specs=(
            P(None, ("gx", "gy")),
            P(("gx", "gy")),
            P(("gx", "gy"), None),
            P(("gx", "gy")),
            P(),
            P("gx", "gy"),
            P(None, "gx", "gy"),
        ),
        out_specs=(P("gx", "gy"), P(None, "gx", "gy")),
        check_vma=False,
    )
```

```python
import functools

import jax
import jax.numpy as jnp
from jax import lax
from jax.experimental import pallas as pl
from jax.experimental.pallas import tpu as pltpu
from jax.sharding import PartitionSpec as P

F32 = jnp.float32
BF16 = jnp.bfloat16
F8 = jnp.float8_e4m3fn
LANES = 128
ROWS = 8
NT = (((1,), (1,)), ((), ()))
MESH = pl.DeviceIdType.MESH


def split(x):
    high = x.astype(BF16).astype(F32)
    return high, x - high


def pick(table, index, axis):
    other = (1 - axis,)
    return lax.gather(
        table,
        index[..., None],
        lax.GatherDimensionNumbers(
            offset_dims=(),
            collapsed_slice_dims=(axis,),
            start_index_map=(axis,),
            operand_batching_dims=other,
            start_indices_batching_dims=other,
        ),
        slice_sizes=(1, 1),
        mode=lax.GatherScatterMode.PROMISE_IN_BOUNDS,
    )


def iota(shape, dim):
    return lax.broadcasted_iota(jnp.int32, shape, dim)


def fused_kernel(
    width_x,
    width_y,
    capacity,
    props_hbm,
    class_hbm,
    owner_hbm,
    cell_hbm,
    table_hbm,
    dens_hbm,
    rest_hbm,
    dens_out,
    rest_out,
    props_ref,
    class_ref,
    owner_ref,
    cell_ref,
    table_ref,
    scalars_ref,
    field,
    flow,
    far_flow,
    hot,
    vals,
    keys,
    packed,
    got,
    spot,
    tab,
    total,
    far_out,
    far_in,
    row_out,
    row_in,
    col_out,
    col_in,
    load_sem,
    send_sem,
    recv_sem,
    far_send,
    far_recv,
    halo_recv,
):
    devices = width_x * width_y
    deep = width_x // 2
    team = deep * width_y
    groups = team // ROWS
    tiles = capacity // LANES
    block = tiles * ROWS
    my_x, my_y = lax.axis_index("gx"), lax.axis_index("gy")
    half = lax.div(my_x, deep)
    row_of = my_x - half * deep
    me = row_of * width_y + my_y
    base_x = half * deep
    mirror = (row_of + (1 - half) * deep, my_y)
    props_count, parcels = props_ref.shape
    classes = table_ref.shape[0]
    slab_x, slab_y = dens_hbm.shape

    def mate(local):
        return (base_x + lax.div(local, width_y), lax.rem(local, width_y))

    loads = [
        pltpu.make_async_copy(a, b, load_sem.at[i])
        for i, (a, b) in enumerate(
            [
                (owner_hbm, owner_ref),
                (dens_hbm, field.at[0]),
                (rest_hbm, field.at[1:5]),
                (table_hbm, table_ref),
                (class_hbm, class_ref),
                (cell_hbm, cell_ref),
                (props_hbm, props_ref),
                (table_hbm, scalars_ref),
            ]
        )
    ]
    for load in loads:
        load.start()

    barrier = pltpu.get_barrier_semaphore()

    def greet(target):
        pl.semaphore_signal(barrier, inc=1, device_id=target, device_id_type=MESH)

    def greet_mate(k, unused):
        greet(mate(lax.rem(me + k, team)))
        return unused

    middle = team // 2
    lax.fori_loop(middle, team, greet_mate, 0, unroll=True if team == 16 else 1)
    greet(mirror)
    last_low = (half == 0) & (row_of == deep - 1)
    first_high = (half == 1) & (row_of == 0)

    @pl.when(last_low)
    def _():
        greet((my_x + 1, my_y))

    @pl.when(first_high)
    def _():
        greet((my_x - 1, my_y))

    around = [
        ((mirror[0] + 1, my_y), row_of < deep - 1),
        ((mirror[0] - 1, my_y), row_of > 0),
        ((mirror[0], my_y + 1), my_y < width_y - 1),
        ((mirror[0], my_y - 1), my_y > 0),
    ]
    greets = team + jnp.where(last_low | first_high, 1, 0)
    for target, there in around:
        greets = greets + jnp.where(there, 1, 0)

        @pl.when(there)
        def _():
            greet(target)

    lax.fori_loop(1, middle, greet_mate, 0, unroll=True if team == 16 else 1)

    def rows_of(local):
        return pl.ds(pl.multiple_of(local * block, ROWS), block)

    def copy_to(phase, local):
        return pltpu.make_async_remote_copy(
            src_ref=packed.at[phase, local],
            dst_ref=got.at[phase, rows_of(me)],
            send_sem=send_sem.at[phase],
            recv_sem=recv_sem.at[phase, lax.div(me, ROWS)],
            device_id=mate(local),
            device_id_type=MESH,
        )

    def wait_blocks(phase, first, count):
        blocks = got.at[phase, pl.ds(pl.multiple_of(first * block, ROWS), count * block)]
        pltpu.make_async_remote_copy(
            src_ref=blocks,
            dst_ref=blocks,
            send_sem=send_sem.at[phase],
            recv_sem=recv_sem.at[phase, lax.div(first, ROWS)],
            device_id=mirror,
            device_id_type=MESH,
        ).wait_recv()

    def far_copy(out_ref, in_ref, i):
        return pltpu.make_async_remote_copy(
            src_ref=out_ref,
            dst_ref=in_ref,
            send_sem=far_send.at[i],
            recv_sem=far_recv.at[i],
            device_id=mirror,
            device_id_type=MESH,
        )

    loads[0].wait()
    row, col = (iota((LANES, 2 * LANES), 0), iota((LANES, 2 * LANES), 1))
    upper = jnp.where((col >= LANES) | (row < col), 1.0, 0.0).astype(BF16)
    ids = iota((devices, LANES), 0)
    wide = hot.shape[0]
    spans = capacity // wide
    ranks = iota((wide, LANES), 0).astype(F32).astype(BF16)
    one, zero = jnp.ones((), BF16), jnp.zeros((), BF16)
    carry = jnp.zeros((devices, LANES), F32)
    chunks = parcels // LANES
    for start in range(0, chunks, ROWS):
        span = range(start, min(start + ROWS, chunks))
        named = [owner_ref[:, c * LANES : (c + 1) * LANES] for c in span]
        mine = [jnp.where(owner == ids, 1.0, 0.0) for owner in named]
        counted = jnp.dot(
            jnp.concatenate(mine, axis=0).astype(BF16), upper, preferred_element_type=F32
        )
        for i, c in enumerate(span):
            part_of = counted[i * devices : (i + 1) * devices]
            rank = jnp.sum(mine[i] * (part_of[:, :LANES] + carry), axis=0, keepdims=True)
            carry = carry + part_of[:, LANES:]
            key = named[i].astype(F32)
            if spans > 1:
                level = sum(jnp.where(rank >= wide * k, 1.0, 0.0) for k in range(1, spans))
                rank = rank - level * wide
                key = key * spans + level
            at = slice(c * LANES, (c + 1) * LANES)
            keys[:, at] = jnp.broadcast_to(key, (2 * ROWS, LANES)).astype(BF16)
            hot[:, at] = jnp.where(ranks == rank.astype(BF16), one, zero).astype(F8)

    for load in loads[1:]:
        load.wait()
    inverse = 1.0 / field[0]
    for c in range(4):
        flow[c] = field[c + 1] * inverse
    eye = jnp.where(
        iota((props_count, props_count), 0) == iota((props_count, props_count), 1), 1.0, 0.0
    ).astype(BF16)
    table = jnp.concatenate(split(table_ref[...]), axis=0).astype(BF16)
    turned = lax.dot_general(eye, table, NT, preferred_element_type=F32).astype(BF16)
    picks = jnp.where(class_ref[...] == iota((classes, parcels), 0), 1.0, 0.0)
    picks = jnp.concatenate([picks, picks], axis=0).astype(BF16)
    coef = jnp.dot(turned, picks, preferred_element_type=F32)
    props = props_ref[...]
    which = iota((props_count, parcels), 0)
    weights = jnp.where(which >= 5, coef, jnp.where(which == 4, 1.0, 0.0))
    heat_sum = jnp.sum(weights * props, axis=0, keepdims=True)
    which = iota((ROWS, parcels), 0)
    mixed = jnp.where(which == 0, jnp.exp(0.5 * props[0:1]), props[0:ROWS])
    mixed = jnp.where(which == 5, heat_sum, mixed)
    mixed = jnp.where(which == 6, class_ref[...].astype(F32), mixed)
    mixed = jnp.where(which == 7, cell_ref[...].astype(F32), mixed)
    vals[...] = jnp.concatenate(split(mixed), axis=0).astype(BF16)

    def first_of(turn):
        return lax.rem(lax.div(me, ROWS) + turn, groups) * ROWS

    def pack(phase, turn):
        first = first_of(turn)
        first_id = (half * team if phase else (1 - half) * team) + first
        count = ROWS * spans // 2
        both = [0.0, 0.0]
        for start in range(0, parcels, 256):
            at = slice(start, start + 256)
            for side in range(2):
                sends = [
                    jnp.where(
                        keys[:, at]
                        == (first_id * spans + side * count + i).astype(F32).astype(BF16),
                        vals[:, at],
                        zero,
                    )
                    for i in range(count)
                ]
                both[side] += lax.dot_general(
                    jnp.concatenate(sends, axis=0),
                    hot[:, at],
                    NT,
                    preferred_element_type=F32,
                )
        both = jnp.concatenate(both, axis=0)
        for i in range(ROWS):
            for k in range(spans):
                at = 2 * ROWS * (i * spans + k)
                whole = both[at : at + ROWS] + both[at + ROWS : at + 2 * ROWS]
                for t in range(wide // LANES):
                    tile = k * (wide // LANES) + t
                    packed[phase, first + i, tile * ROWS : (tile + 1) * ROWS] = whole[
                        :, t * LANES : (t + 1) * LANES
                    ]

    def launch(phase, turn, near):
        for i in range(1, ROWS if near else ROWS + 1):
            copy_to(phase, first_of(turn) + lax.rem(me + i, ROWS)).start()

    def send(phase, turn, near):
        pack(phase, turn)
        launch(phase, turn, near)

    def send_others(phase, start):
        if groups - start <= 2:
            for turn in range(start, groups):
                send(phase, turn, False)
        else:
            lax.fori_loop(start, groups, lambda k, u: (send(phase, k, False), u)[1], 0)

    early = row_of * 2 < deep
    pack(0, 0)
    if groups > 1:
        pack(0, 1)
    pl.semaphore_wait(barrier, greets)

    @pl.when(early)
    def _():
        far_copy(flow, far_flow, 0).start()

    launch(0, 0, True)
    if groups > 1:
        launch(0, 1, False)
        send_others(0, 2)

    @pl.when(jnp.logical_not(early))
    def _():
        far_copy(flow, far_flow, 0).start()

    send(1, 0, True)
    send_others(1, 1)
    for phase in range(2):
        got[phase, rows_of(me)] = packed[phase, me]

    half_x = slab_x // 2
    ys = iota((2 * slab_y, capacity), 0).astype(F32).astype(BF16)
    xs_short = iota((half_x, capacity), 0).astype(F32).astype(BF16)
    sub = iota((ROWS, LANES), 0)

    def prepare(phase, fields):
        parts = []
        for c in range(4):
            for piece in split(fields[c]):
                parts.append(jnp.concatenate([piece[:half_x], piece[half_x:]], axis=1))
        tab[phase] = jnp.concatenate(parts, axis=0).astype(BF16)

    def take_group(phase, turn):
        if True:
            first = first_of(turn)

            @pl.when(turn == 0)
            def _():
                wait_blocks(phase, first, ROWS - 1)

            @pl.when(turn != 0)
            def _():
                wait_blocks(phase, first, ROWS)

            def part(c):
                return jnp.concatenate(
                    [
                        got[phase, pl.ds(first * block + t * ROWS + c, ROWS, stride=block), :]
                        for t in range(tiles)
                    ],
                    axis=1,
                )

            cell = part(7).astype(jnp.int32)
            line = lax.div(cell, slab_y)
            lane_of = cell - line * slab_y
            upper_half = jnp.where(line >= half_x, 1, 0)
            lanes_at = (lane_of + upper_half * slab_y).astype(F32)
            lines_short = (line - upper_half * half_x).astype(F32)
            line_at = line - upper_half * half_x
            shelf = lax.div(line_at, ROWS)
            within = line_at - shelf * ROWS
            gas = [[jnp.zeros((ROWS, LANES), F32)] * tiles for c in range(4)]
            for i in range(ROWS):
                spot_at = slice(i * capacity, (i + 1) * capacity)
                spot[:, spot_at] = jnp.where(
                    ys == lanes_at[i : i + 1].astype(BF16), one, zero
                ).astype(F8)
                found = jnp.dot(tab[phase], spot[:, spot_at], preferred_element_type=F32)
                for t in range(tiles):
                    lanes = slice(t * LANES, (t + 1) * LANES)
                    low, deep_row = [
                        jnp.broadcast_to(x[i : i + 1, lanes], (ROWS, LANES))
                        for x in (within, shelf)
                    ]
                    for c in range(4):
                        pieces = []
                        for p in range(2):
                            at = (2 * c + p) * half_x
                            piece = found[at : at + ROWS, lanes]
                            for r in range(1, half_x // ROWS):
                                here = found[at + r * ROWS : at + (r + 1) * ROWS, lanes]
                                piece = jnp.where(deep_row >= r, here, piece)
                            pieces.append(piece)
                        gas[c][t] = jnp.where(
                            sub == i, pick(pieces[0] + pieces[1], low, 0), gas[c][t]
                        )
            gas = [jnp.concatenate(row, axis=1) for row in gas]

            kind = part(6).astype(jnp.int32)
            coefs = [jnp.full(kind.shape, scalars_ref[0, j], F32) for j in range(5)]
            for k in range(1, classes):
                same = kind == k
                coefs = [jnp.where(same, scalars_ref[k, j], coefs[j]) for j in range(5)]
            mass = part(0)
            speed = [part(j) for j in (1, 2, 3)]
            heat, energy = part(4), part(5)
            slip = [speed[j] - gas[j] for j in range(3)]
            excess = heat - gas[3]
            soft = jnp.maximum(excess, 0.0) + jnp.log1p(jnp.exp(-jnp.abs(excess)))
            evapor = mass * (1.0 - jnp.exp(-(coefs[0] * soft)))
            square = slip[0] * slip[0] + slip[1] * slip[1] + slip[2] * slip[2]
            drag = mass * (1.0 - jnp.exp(-coefs[1] * jnp.sqrt(1.0 + square)))
            out = [evapor]
            out += [evapor * coefs[2 + j] * speed[j] + drag * slip[j] for j in range(3)]
            out += [evapor * energy]

            pieces = [piece for c in range(5) for piece in split(out[c])]
            spread = []
            for i in range(ROWS):
                in_row = xs_short == lines_short[i : i + 1].astype(BF16)
                spread.append(
                    jnp.concatenate(
                        [
                            jnp.where(in_row, piece[i : i + 1].astype(BF16), zero)
                            for piece in pieces
                        ],
                        axis=0,
                    )
                )
            for side in range(2):
                at = side * ROWS // 2
                total[phase, side] += lax.dot_general(
                    jnp.concatenate(spread[at : at + ROWS // 2], axis=1),
                    spot[:, at * capacity : (at + ROWS // 2) * capacity],
                    NT,
                    preferred_element_type=F32,
                )

    def deposit_of(phase):
        whole = total[phase, 0] + total[phase, 1]
        summed = []
        for c in range(5):
            at = 2 * c * half_x
            both = whole[at : at + half_x] + whole[at + half_x : at + 2 * half_x]
            summed.append(jnp.concatenate([both[:, :slab_y], both[:, slab_y:]], axis=0))
        return summed

    lane = iota((slab_x, slab_y), 1)

    def edges_of(origin):
        x, y = origin
        return [
            (row_out, row_in, 0, 0, (x - 1, y), x > 0, my_x < width_x - 1),
            (row_out, row_in, 1, 0, (x + 1, y), x < width_x - 1, my_x > 0),
            (col_out, col_in, 0, 2, (x, y - 1), y > 0, my_y < width_y - 1),
            (col_out, col_in, 1, 2, (x, y + 1), y < width_y - 1, my_y > 0),
        ]

    def edge(phase, out_ref, in_ref, side, base, target):
        at = 4 * phase + base + side
        return pltpu.make_async_remote_copy(
            src_ref=out_ref.at[phase, side],
            dst_ref=in_ref.at[phase, side],
            send_sem=load_sem.at[at],
            recv_sem=halo_recv.at[at],
            device_id=target,
            device_id_type=MESH,
        )

    origins = (mirror, (my_x, my_y))

    def send_edges(phase, deposit):
        sides = jnp.zeros((slab_x, slab_y), F32)
        for c in range(5):
            row_out[phase, 0, c : c + 1] = deposit[c][0:1]
            row_out[phase, 1, c : c + 1] = deposit[c][slab_x - 1 : slab_x]
            first = pltpu.roll(deposit[c], c, 1) if c else deposit[c]
            sides = jnp.where(lane == c, first, sides)
            last = pltpu.roll(deposit[c], ROWS + c + 1, 1)
            sides = jnp.where(lane == ROWS + c, last, sides)
        turned = jnp.transpose(sides)
        for side in range(2):
            col_out[phase, side, :, :slab_x] = turned[side * ROWS : (side + 1) * ROWS]
        for out_ref, in_ref, side, base, target, sends, takes in edges_of(origins[phase]):

            @pl.when(sends)
            def _():
                edge(phase, out_ref, in_ref, side, base, target).start()

    for ref in (row_out, col_out):
        ref[...] = jnp.zeros_like(ref)
    for out_ref, in_ref, side, base, target, sends, takes in edges_of(origins[1]):

        @pl.when(jnp.logical_not(takes))
        def _():
            for phase in range(2):
                in_ref[phase, side] = jnp.zeros(in_ref.shape[2:], F32)

    total[...] = jnp.zeros_like(total)
    prepare(1, flow)
    own_first = (half == 0) & jnp.logical_not(early)
    lead = jnp.where(own_first if groups == 1 else half == 0, 1, 0)

    hold = jnp.where((half == 1) & jnp.logical_not(early), min(groups, 2), 0)

    def step(t, unused):
        head = (lead == 1) & (t < 2)
        far_turn = jnp.where(
            head, jnp.where(own_first, t, 1 - t), jnp.where(t < groups + lead, 1, 0)
        )
        turn = jnp.where(head, 0, jnp.where(far_turn == 1, t - lead, t - groups))

        @pl.when(t == jnp.where(own_first, 1, 0))
        def _():
            far_copy(flow, far_flow, 0).wait_recv()
            prepare(0, far_flow)

        take_group(1 - far_turn, turn)

        @pl.when(t == groups - 1 + lead)
        def _():
            deposit = deposit_of(0)
            for c in range(5):
                far_out[c] = deposit[c]
            send_edges(0, deposit)

        @pl.when(t == groups - 1 + lead + hold)
        def _():
            far_copy(far_out, far_in, 1).start()

        return unused

    lax.fori_loop(0, 2 * groups, step, 0)
    mine = deposit_of(1)
    send_edges(1, mine)
    for phase in range(2):
        blocks = packed.at[phase, pl.ds(0, team - 1)]
        pltpu.make_async_remote_copy(
            src_ref=blocks,
            dst_ref=blocks,
            send_sem=send_sem.at[phase],
            recv_sem=recv_sem.at[phase, 0],
            device_id=mirror,
            device_id_type=MESH,
        ).wait_send()
    far_copy(flow, far_flow, 0).wait_send()
    far_copy(far_out, far_in, 1).wait_send()
    far_copy(far_out, far_in, 1).wait_recv()
    for phase in range(2):
        for out_ref, in_ref, side, base, target, sends, takes in edges_of(origins[1]):

            @pl.when(takes)
            def _():
                edge(phase, out_ref, in_ref, side, base, target).wait_recv()

    rows_in = [row_in[0, side] + row_in[1, side] for side in range(2)]
    cols_in = [
        jnp.transpose(col_in[0, side] + col_in[1, side])[:slab_x] for side in range(2)
    ]
    for c in range(5):
        here = mine[c] + far_in[c]
        above = jnp.concatenate([rows_in[1][c : c + 1], here[: slab_x - 1]], axis=0)
        below = jnp.concatenate([here[1:], rows_in[0][c : c + 1]], axis=0)
        beside = [jnp.broadcast_to(x[:, c : c + 1], (slab_x, slab_y)) for x in cols_in]
        left = jnp.where(lane == 0, beside[1], pltpu.roll(here, 1, 1))
        right = jnp.where(lane == slab_y - 1, beside[0], pltpu.roll(here, slab_y - 1, 1))
        smooth = 0.4 * here + 0.15 * (below + above + right + left)
        if c:
            rest_out[c - 1] = field[c] + smooth
        else:
            dens_out[...] = field[0] + smooth

    for phase in range(2):
        for out_ref, in_ref, side, base, target, sends, takes in edges_of(origins[phase]):

            @pl.when(sends)
            def _():
                edge(phase, out_ref, in_ref, side, base, target).wait_send()


def per_device(
    parcel_props, size_class, dest_owner, dest_local, class_table, gas_density, gas_rest
):
    width_x, width_y = lax.axis_size("gx"), lax.axis_size("gy")
    devices = width_x * width_y
    team = devices // 2
    props_count, parcels = parcel_props.shape
    slab_x, slab_y = gas_density.shape
    capacity = -(-max(2, 4 * parcels // devices) // LANES) * LANES
    hbm = pl.BlockSpec(memory_space=pl.ANY)
    vmem = pl.BlockSpec(memory_space=pltpu.VMEM)
    dens, rest = pl.pallas_call(
        functools.partial(fused_kernel, width_x, width_y, capacity),
        out_shape=(
            pltpu.VMEM((slab_x, slab_y), F32),
            pltpu.VMEM((4, slab_x, slab_y), F32),
        ),
        in_specs=[hbm] * 7,
        out_specs=(vmem, vmem),
        scratch_shapes=[
            pltpu.VMEM((props_count, parcels), F32),
            pltpu.VMEM((1, parcels), jnp.int32),
            pltpu.VMEM((1, parcels), jnp.int32),
            pltpu.VMEM((1, parcels), jnp.int32),
            pltpu.VMEM(class_table.shape, F32),
            pltpu.SMEM(class_table.shape, F32),
            pltpu.VMEM((5, slab_x, slab_y), F32),
            pltpu.VMEM((4, slab_x, slab_y), F32),
            pltpu.VMEM((4, slab_x, slab_y), F32),
            pltpu.VMEM((min(capacity, 256), parcels), F8),
            pltpu.VMEM((2 * ROWS, parcels), BF16),
            pltpu.VMEM((2 * ROWS, parcels), BF16),
            pltpu.VMEM((2, team, capacity // LANES * ROWS, LANES), F32),
            pltpu.VMEM((2, team * capacity // LANES * ROWS, LANES), F32),
            pltpu.VMEM((2 * slab_y, ROWS * capacity), F8),
            pltpu.VMEM((2, 4 * slab_x, 2 * slab_y), BF16),
            pltpu.VMEM((2, 2, 5 * slab_x, 2 * slab_y), F32),
            pltpu.VMEM((5, slab_x, slab_y), F32),
            pltpu.VMEM((5, slab_x, slab_y), F32),
            pltpu.VMEM((2, 2, ROWS, slab_y), F32),
            pltpu.VMEM((2, 2, ROWS, slab_y), F32),
            pltpu.VMEM((2, 2, ROWS, LANES), F32),
            pltpu.VMEM((2, 2, ROWS, LANES), F32),
            pltpu.SemaphoreType.DMA((8,)),
            pltpu.SemaphoreType.DMA((2,)),
            pltpu.SemaphoreType.DMA((2, team // ROWS)),
            pltpu.SemaphoreType.DMA((2,)),
            pltpu.SemaphoreType.DMA((2,)),
            pltpu.SemaphoreType.DMA((8,)),
        ],
        compiler_params=pltpu.CompilerParams(collective_id=0, has_side_effects=True),
    )(
        parcel_props,
        size_class.reshape(1, parcels),
        dest_owner.reshape(1, parcels),
        dest_local.reshape(1, parcels),
        class_table,
        gas_density,
        gas_rest,
    )
    return pl.pallas_call(
        store_kernel,
        out_shape=(
            jax.ShapeDtypeStruct(dens.shape, F32),
            jax.ShapeDtypeStruct(rest.shape, F32),
        ),
        in_specs=[hbm, hbm],
        out_specs=(hbm, hbm),
        scratch_shapes=[pltpu.SemaphoreType.DMA((2,))],
    )(*(pltpu.with_memory_space_constraint(x, pltpu.VMEM) for x in (dens, rest)))


def store_kernel(dens_ref, rest_ref, dens_out, rest_out, sem):
    stores = [
        pltpu.make_async_copy(dens_ref, dens_out, sem.at[0]),
        pltpu.make_async_copy(rest_ref, rest_out, sem.at[1]),
    ]
    for store in stores:
        store.start()
    for store in stores:
        store.wait()


def solution(mesh):
    return jax.shard_map(
        per_device,
        mesh=mesh,
        in_specs=(
            P(None, ("gx", "gy")),
            P(("gx", "gy")),
            P(("gx", "gy"), None),
            P(("gx", "gy")),
            P(),
            P("gx", "gy"),
            P(None, "gx", "gy"),
        ),
        out_specs=(P("gx", "gy"), P(None, "gx", "gy")),
        check_vma=False,
    )
```

```python
import functools

import jax
import jax.numpy as jnp
from jax import lax
from jax.experimental import pallas as pl
from jax.experimental.pallas import tpu as pltpu
from jax.sharding import PartitionSpec as P

F32 = jnp.float32
BF16 = jnp.bfloat16
F8 = jnp.float8_e4m3fn
LANES = 128
ROWS = 8
NT = (((1,), (1,)), ((), ()))
MESH = pl.DeviceIdType.MESH


def split(x):
    high = x.astype(BF16).astype(F32)
    return high, x - high


def pick(table, index, axis):
    other = (1 - axis,)
    return lax.gather(
        table,
        index[..., None],
        lax.GatherDimensionNumbers(
            offset_dims=(),
            collapsed_slice_dims=(axis,),
            start_index_map=(axis,),
            operand_batching_dims=other,
            start_indices_batching_dims=other,
        ),
        slice_sizes=(1, 1),
        mode=lax.GatherScatterMode.PROMISE_IN_BOUNDS,
    )


def iota(shape, dim):
    return lax.broadcasted_iota(jnp.int32, shape, dim)


def fused_kernel(
    width_x,
    width_y,
    capacity,
    props_hbm,
    class_hbm,
    owner_hbm,
    cell_hbm,
    table_hbm,
    dens_hbm,
    rest_hbm,
    dens_out,
    rest_out,
    props_ref,
    class_ref,
    owner_ref,
    cell_ref,
    table_ref,
    scalars_ref,
    field,
    flow,
    far_flow,
    hot,
    vals,
    keys,
    packed,
    got,
    spot,
    tab,
    total,
    far_out,
    far_in,
    row_out,
    row_in,
    col_out,
    col_in,
    load_sem,
    send_sem,
    recv_sem,
    far_send,
    far_recv,
    halo_recv,
):
    devices = width_x * width_y
    deep = width_x // 2
    team = deep * width_y
    groups = team // ROWS
    tiles = capacity // LANES
    block = tiles * ROWS
    my_x, my_y = lax.axis_index("gx"), lax.axis_index("gy")
    half = lax.div(my_x, deep)
    row_of = my_x - half * deep
    me = row_of * width_y + my_y
    base_x = half * deep
    mirror = (row_of + (1 - half) * deep, my_y)
    props_count, parcels = props_ref.shape
    classes = table_ref.shape[0]
    slab_x, slab_y = dens_hbm.shape

    def mate(local):
        return (base_x + lax.div(local, width_y), lax.rem(local, width_y))

    loads = [
        pltpu.make_async_copy(a, b, load_sem.at[i])
        for i, (a, b) in enumerate(
            [
                (owner_hbm, owner_ref),
                (dens_hbm, field.at[0]),
                (rest_hbm, field.at[1:5]),
                (table_hbm, table_ref),
                (class_hbm, class_ref),
                (cell_hbm, cell_ref),
                (props_hbm, props_ref),
                (table_hbm, scalars_ref),
            ]
        )
    ]
    for load in loads:
        load.start()

    barrier = pltpu.get_barrier_semaphore()

    def greet(target):
        pl.semaphore_signal(barrier, inc=1, device_id=target, device_id_type=MESH)

    def greet_mate(k, unused):
        greet(mate(lax.rem(me + k, team)))
        return unused

    middle = team // 2
    lax.fori_loop(middle, team, greet_mate, 0, unroll=True if team == 16 else 1)
    greet(mirror)
    last_low = (half == 0) & (row_of == deep - 1)
    first_high = (half == 1) & (row_of == 0)

    @pl.when(last_low)
    def _():
        greet((my_x + 1, my_y))

    @pl.when(first_high)
    def _():
        greet((my_x - 1, my_y))

    around = [
        ((mirror[0] + 1, my_y), row_of < deep - 1),
        ((mirror[0] - 1, my_y), row_of > 0),
        ((mirror[0], my_y + 1), my_y < width_y - 1),
        ((mirror[0], my_y - 1), my_y > 0),
    ]
    greets = team + jnp.where(last_low | first_high, 1, 0)
    for target, there in around:
        greets = greets + jnp.where(there, 1, 0)

        @pl.when(there)
        def _():
            greet(target)

    lax.fori_loop(1, middle, greet_mate, 0, unroll=True if team == 16 else 1)

    def rows_of(local):
        return pl.ds(pl.multiple_of(local * block, ROWS), block)

    def copy_to(phase, local):
        return pltpu.make_async_remote_copy(
            src_ref=packed.at[phase, local],
            dst_ref=got.at[phase, rows_of(me)],
            send_sem=send_sem.at[phase],
            recv_sem=recv_sem.at[phase, lax.div(me, ROWS)],
            device_id=mate(local),
            device_id_type=MESH,
        )

    def wait_blocks(phase, first, count):
        blocks = got.at[phase, pl.ds(pl.multiple_of(first * block, ROWS), count * block)]
        pltpu.make_async_remote_copy(
            src_ref=blocks,
            dst_ref=blocks,
            send_sem=send_sem.at[phase],
            recv_sem=recv_sem.at[phase, lax.div(first, ROWS)],
            device_id=mirror,
            device_id_type=MESH,
        ).wait_recv()

    def far_copy(out_ref, in_ref, i):
        return pltpu.make_async_remote_copy(
            src_ref=out_ref,
            dst_ref=in_ref,
            send_sem=far_send.at[i],
            recv_sem=far_recv.at[i],
            device_id=mirror,
            device_id_type=MESH,
        )

    loads[0].wait()
    row, col = (iota((LANES, 2 * LANES), 0), iota((LANES, 2 * LANES), 1))
    upper = jnp.where((col >= LANES) | (row < col), 1.0, 0.0).astype(BF16)
    ids = iota((devices, LANES), 0)
    wide = hot.shape[0]
    spans = capacity // wide
    ranks = iota((wide, LANES), 0).astype(F32).astype(BF16)
    one, zero = jnp.ones((), BF16), jnp.zeros((), BF16)
    carry = jnp.zeros((devices, LANES), F32)
    chunks = parcels // LANES
    for start in range(0, chunks, ROWS):
        span = range(start, min(start + ROWS, chunks))
        named = [owner_ref[:, c * LANES : (c + 1) * LANES] for c in span]
        mine = [jnp.where(owner == ids, 1.0, 0.0) for owner in named]
        counted = jnp.dot(
            jnp.concatenate(mine, axis=0).astype(BF16), upper, preferred_element_type=F32
        )
        for i, c in enumerate(span):
            part_of = counted[i * devices : (i + 1) * devices]
            rank = jnp.sum(mine[i] * (part_of[:, :LANES] + carry), axis=0, keepdims=True)
            carry = carry + part_of[:, LANES:]
            key = named[i].astype(F32)
            if spans > 1:
                level = sum(jnp.where(rank >= wide * k, 1.0, 0.0) for k in range(1, spans))
                rank = rank - level * wide
                key = key * spans + level
            at = slice(c * LANES, (c + 1) * LANES)
            keys[:, at] = jnp.broadcast_to(key, (2 * ROWS, LANES)).astype(BF16)
            hot[:, at] = jnp.where(ranks == rank.astype(BF16), one, zero).astype(F8)

    for load in loads[1:]:
        load.wait()
    inverse = 1.0 / field[0]
    for c in range(4):
        flow[c] = field[c + 1] * inverse
    eye = jnp.where(
        iota((props_count, props_count), 0) == iota((props_count, props_count), 1), 1.0, 0.0
    ).astype(BF16)
    table = jnp.concatenate(split(table_ref[...]), axis=0).astype(BF16)
    turned = lax.dot_general(eye, table, NT, preferred_element_type=F32).astype(BF16)
    picks = jnp.where(class_ref[...] == iota((classes, parcels), 0), 1.0, 0.0)
    picks = jnp.concatenate([picks, picks], axis=0).astype(BF16)
    coef = jnp.dot(turned, picks, preferred_element_type=F32)
    props = props_ref[...]
    which = iota((props_count, parcels), 0)
    weights = jnp.where(which >= 5, coef, jnp.where(which == 4, 1.0, 0.0))
    heat_sum = jnp.sum(weights * props, axis=0, keepdims=True)
    which = iota((ROWS, parcels), 0)
    mixed = jnp.where(which == 0, jnp.exp(0.5 * props[0:1]), props[0:ROWS])
    mixed = jnp.where(which == 5, heat_sum, mixed)
    mixed = jnp.where(which == 6, class_ref[...].astype(F32), mixed)
    mixed = jnp.where(which == 7, cell_ref[...].astype(F32), mixed)
    vals[...] = jnp.concatenate(split(mixed), axis=0).astype(BF16)

    def first_of(turn):
        return lax.rem(lax.div(me, ROWS) + turn, groups) * ROWS

    def pack(phase, turn):
        first = first_of(turn)
        first_id = jnp.where(phase == half, team, 0) + first
        count = ROWS * spans // 2
        both = [0.0, 0.0]
        for start in range(0, parcels, 256):
            at = slice(start, start + 256)
            for side in range(2):
                sends = [
                    jnp.where(
                        keys[:, at]
                        == (first_id * spans + side * count + i).astype(F32).astype(BF16),
                        vals[:, at],
                        zero,
                    )
                    for i in range(count)
                ]
                both[side] += lax.dot_general(
                    jnp.concatenate(sends, axis=0),
                    hot[:, at],
                    NT,
                    preferred_element_type=F32,
                )
        both = jnp.concatenate(both, axis=0)
        for i in range(ROWS):
            for k in range(spans):
                at = 2 * ROWS * (i * spans + k)
                whole = both[at : at + ROWS] + both[at + ROWS : at + 2 * ROWS]
                for t in range(wide // LANES):
                    tile = k * (wide // LANES) + t
                    packed[phase, first + i, tile * ROWS : (tile + 1) * ROWS] = whole[
                        :, t * LANES : (t + 1) * LANES
                    ]

    def launch(phase, turn, near):
        for i in range(1, ROWS if near else ROWS + 1):
            copy_to(phase, first_of(turn) + lax.rem(me + i, ROWS)).start()

    def send(phase, turn, near):
        pack(phase, turn)
        launch(phase, turn, near)

    def send_others(phase, start):
        if groups - start <= 2:
            for turn in range(start, groups):
                send(phase, turn, False)
        else:
            lax.fori_loop(start, groups, lambda k, u: (send(phase, k, False), u)[1], 0)

    early = row_of * 2 < deep
    low = jnp.where(half == 0, 1, 0)
    low_inner = jnp.where((half == 0) & jnp.logical_not(early), 1, 0)
    low_outer = low - low_inner
    pack(low_inner, 0)
    if groups > 1:
        pack(low_outer, 1)
    pl.semaphore_wait(barrier, greets)

    @pl.when(early)
    def _():
        far_copy(flow, far_flow, 0).start()

    launch(low_inner, 0, True)
    if groups > 1:
        launch(low_outer, 1, False)
        send_others(low_outer, 2)

    @pl.when(jnp.logical_not(early))
    def _():
        far_copy(flow, far_flow, 0).start()

    @pl.when(low_outer == 1)
    def _():
        send(1, 0, True)
        send_others(0, 1)

    @pl.when(low_outer == 0)
    def _():
        send_others(1, 1)
        send(1 - low_inner, 0, True)

    for phase in range(2):
        got[phase, rows_of(me)] = packed[phase, me]

    half_x = slab_x // 2
    ys = iota((2 * slab_y, capacity), 0).astype(F32).astype(BF16)
    xs_short = iota((half_x, capacity), 0).astype(F32).astype(BF16)
    sub = iota((ROWS, LANES), 0)

    def prepare(phase, fields):
        parts = []
        for c in range(4):
            for piece in split(fields[c]):
                parts.append(jnp.concatenate([piece[:half_x], piece[half_x:]], axis=1))
        tab[phase] = jnp.concatenate(parts, axis=0).astype(BF16)

    def take_group(phase, turn):
        if True:
            first = first_of(turn)

            @pl.when(turn == 0)
            def _():
                wait_blocks(phase, first, ROWS - 1)

            @pl.when(turn != 0)
            def _():
                wait_blocks(phase, first, ROWS)

            def part(c):
                return jnp.concatenate(
                    [
                        got[phase, pl.ds(first * block + t * ROWS + c, ROWS, stride=block), :]
                        for t in range(tiles)
                    ],
                    axis=1,
                )

            cell = part(7).astype(jnp.int32)
            line = lax.div(cell, slab_y)
            lane_of = cell - line * slab_y
            upper_half = jnp.where(line >= half_x, 1, 0)
            lanes_at = (lane_of + upper_half * slab_y).astype(F32)
            lines_short = (line - upper_half * half_x).astype(F32)
            line_at = line - upper_half * half_x
            shelf = lax.div(line_at, ROWS)
            within = line_at - shelf * ROWS
            gas = [[jnp.zeros((ROWS, LANES), F32)] * tiles for c in range(4)]
            for i in range(ROWS):
                spot_at = slice(i * capacity, (i + 1) * capacity)
                spot[:, spot_at] = jnp.where(
                    ys == lanes_at[i : i + 1].astype(BF16), one, zero
                ).astype(F8)
                found = jnp.dot(tab[phase], spot[:, spot_at], preferred_element_type=F32)
                for t in range(tiles):
                    lanes = slice(t * LANES, (t + 1) * LANES)
                    low, deep_row = [
                        jnp.broadcast_to(x[i : i + 1, lanes], (ROWS, LANES))
                        for x in (within, shelf)
                    ]
                    for c in range(4):
                        pieces = []
                        for p in range(2):
                            at = (2 * c + p) * half_x
                            piece = found[at : at + ROWS, lanes]
                            for r in range(1, half_x // ROWS):
                                here = found[at + r * ROWS : at + (r + 1) * ROWS, lanes]
                                piece = jnp.where(deep_row >= r, here, piece)
                            pieces.append(piece)
                        gas[c][t] = jnp.where(
                            sub == i, pick(pieces[0] + pieces[1], low, 0), gas[c][t]
                        )
            gas = [jnp.concatenate(row, axis=1) for row in gas]

            kind = part(6).astype(jnp.int32)
            coefs = [jnp.full(kind.shape, scalars_ref[0, j], F32) for j in range(5)]
            for k in range(1, classes):
                same = kind == k
                coefs = [jnp.where(same, scalars_ref[k, j], coefs[j]) for j in range(5)]
            mass = part(0)
            speed = [part(j) for j in (1, 2, 3)]
            heat, energy = part(4), part(5)
            slip = [speed[j] - gas[j] for j in range(3)]
            excess = heat - gas[3]
            soft = jnp.maximum(excess, 0.0) + jnp.log1p(jnp.exp(-jnp.abs(excess)))
            evapor = mass * (1.0 - jnp.exp(-(coefs[0] * soft)))
            square = slip[0] * slip[0] + slip[1] * slip[1] + slip[2] * slip[2]
            drag = mass * (1.0 - jnp.exp(-coefs[1] * jnp.sqrt(1.0 + square)))
            out = [evapor]
            out += [evapor * coefs[2 + j] * speed[j] + drag * slip[j] for j in range(3)]
            out += [evapor * energy]

            pieces = [piece for c in range(5) for piece in split(out[c])]
            spread = []
            for i in range(ROWS):
                in_row = xs_short == lines_short[i : i + 1].astype(BF16)
                spread.append(
                    jnp.concatenate(
                        [
                            jnp.where(in_row, piece[i : i + 1].astype(BF16), zero)
                            for piece in pieces
                        ],
                        axis=0,
                    )
                )
            for side in range(2):
                at = side * ROWS // 2
                total[phase, side] += lax.dot_general(
                    jnp.concatenate(spread[at : at + ROWS // 2], axis=1),
                    spot[:, at * capacity : (at + ROWS // 2) * capacity],
                    NT,
                    preferred_element_type=F32,
                )

    def deposit_of(phase):
        whole = total[phase, 0] + total[phase, 1]
        summed = []
        for c in range(5):
            at = 2 * c * half_x
            both = whole[at : at + half_x] + whole[at + half_x : at + 2 * half_x]
            summed.append(jnp.concatenate([both[:, :slab_y], both[:, slab_y:]], axis=0))
        return summed

    lane = iota((slab_x, slab_y), 1)

    def edges_of(origin):
        x, y = origin
        return [
            (row_out, row_in, 0, 0, (x - 1, y), x > 0, my_x < width_x - 1),
            (row_out, row_in, 1, 0, (x + 1, y), x < width_x - 1, my_x > 0),
            (col_out, col_in, 0, 2, (x, y - 1), y > 0, my_y < width_y - 1),
            (col_out, col_in, 1, 2, (x, y + 1), y < width_y - 1, my_y > 0),
        ]

    def edge(phase, out_ref, in_ref, side, base, target):
        at = 4 * phase + base + side
        return pltpu.make_async_remote_copy(
            src_ref=out_ref.at[phase, side],
            dst_ref=in_ref.at[phase, side],
            send_sem=load_sem.at[at],
            recv_sem=halo_recv.at[at],
            device_id=target,
            device_id_type=MESH,
        )

    origins = (mirror, (my_x, my_y))

    def send_edges(phase, deposit):
        sides = jnp.zeros((slab_x, slab_y), F32)
        for c in range(5):
            row_out[phase, 0, c : c + 1] = deposit[c][0:1]
            row_out[phase, 1, c : c + 1] = deposit[c][slab_x - 1 : slab_x]
            first = pltpu.roll(deposit[c], c, 1) if c else deposit[c]
            sides = jnp.where(lane == c, first, sides)
            last = pltpu.roll(deposit[c], ROWS + c + 1, 1)
            sides = jnp.where(lane == ROWS + c, last, sides)
        turned = jnp.transpose(sides)
        for side in range(2):
            col_out[phase, side, :, :slab_x] = turned[side * ROWS : (side + 1) * ROWS]
        for out_ref, in_ref, side, base, target, sends, takes in edges_of(origins[phase]):

            @pl.when(sends)
            def _():
                edge(phase, out_ref, in_ref, side, base, target).start()

    for ref in (row_out, col_out):
        ref[...] = jnp.zeros_like(ref)
    for out_ref, in_ref, side, base, target, sends, takes in edges_of(origins[1]):

        @pl.when(jnp.logical_not(takes))
        def _():
            for phase in range(2):
                in_ref[phase, side] = jnp.zeros(in_ref.shape[2:], F32)

    total[...] = jnp.zeros_like(total)
    prepare(1, flow)
    far_start = low_inner * groups
    far_stop = groups - 1 + low_outer + low_inner * groups
    own_stop = 2 * groups - 1 - low_inner * groups
    if groups == 1:
        far_stop, own_stop = low_inner, 1 - low_inner

    hold = jnp.where((half == 1) & jnp.logical_not(early), min(groups, 2), 0)

    def step(t, unused):
        head = (low_outer == 1) & (t < 2)
        ahead = jnp.where(t < groups + low_outer, 1, 0)
        far_turn = jnp.where(head, 1 - t, jnp.where(low_inner == 1, 1 - ahead, ahead))
        turn = jnp.where(head, 0, jnp.where(ahead == 1, t - low_outer, t - groups))

        @pl.when(t == far_start)
        def _():
            far_copy(flow, far_flow, 0).wait_recv()
            prepare(0, far_flow)

        take_group(1 - far_turn, turn)

        @pl.when(t == far_stop)
        def _():
            deposit = deposit_of(0)
            for c in range(5):
                far_out[c] = deposit[c]
            send_edges(0, deposit)

        @pl.when(t == own_stop)
        def _():
            send_edges(1, deposit_of(1))

        @pl.when(t == far_stop + hold)
        def _():
            far_copy(far_out, far_in, 1).start()

        return unused

    lax.fori_loop(0, 2 * groups, step, 0)
    mine = deposit_of(1)
    far_copy(far_out, far_in, 1).wait_recv()
    for phase in range(2):
        for out_ref, in_ref, side, base, target, sends, takes in edges_of(origins[1]):

            @pl.when(takes)
            def _():
                edge(phase, out_ref, in_ref, side, base, target).wait_recv()

    rows_in = [row_in[0, side] + row_in[1, side] for side in range(2)]
    cols_in = [
        jnp.transpose(col_in[0, side] + col_in[1, side])[:slab_x] for side in range(2)
    ]
    for c in range(5):
        here = mine[c] + far_in[c]
        above = jnp.concatenate([rows_in[1][c : c + 1], here[: slab_x - 1]], axis=0)
        below = jnp.concatenate([here[1:], rows_in[0][c : c + 1]], axis=0)
        beside = [jnp.broadcast_to(x[:, c : c + 1], (slab_x, slab_y)) for x in cols_in]
        left = jnp.where(lane == 0, beside[1], pltpu.roll(here, 1, 1))
        right = jnp.where(lane == slab_y - 1, beside[0], pltpu.roll(here, slab_y - 1, 1))
        smooth = 0.4 * here + 0.15 * (below + above + right + left)
        if c:
            rest_out[c - 1] = field[c] + smooth
        else:
            dens_out[...] = field[0] + smooth

    for phase in range(2):
        blocks = packed.at[phase, pl.ds(0, team - 1)]
        pltpu.make_async_remote_copy(
            src_ref=blocks,
            dst_ref=blocks,
            send_sem=send_sem.at[phase],
            recv_sem=recv_sem.at[phase, 0],
            device_id=mirror,
            device_id_type=MESH,
        ).wait_send()
    far_copy(flow, far_flow, 0).wait_send()
    far_copy(far_out, far_in, 1).wait_send()
    for phase in range(2):
        for out_ref, in_ref, side, base, target, sends, takes in edges_of(origins[phase]):

            @pl.when(sends)
            def _():
                edge(phase, out_ref, in_ref, side, base, target).wait_send()


def per_device(
    parcel_props, size_class, dest_owner, dest_local, class_table, gas_density, gas_rest
):
    width_x, width_y = lax.axis_size("gx"), lax.axis_size("gy")
    devices = width_x * width_y
    team = devices // 2
    props_count, parcels = parcel_props.shape
    slab_x, slab_y = gas_density.shape
    capacity = -(-max(2, 4 * parcels // devices) // LANES) * LANES
    hbm = pl.BlockSpec(memory_space=pl.ANY)
    vmem = pl.BlockSpec(memory_space=pltpu.VMEM)
    dens, rest = pl.pallas_call(
        functools.partial(fused_kernel, width_x, width_y, capacity),
        out_shape=(
            pltpu.VMEM((slab_x, slab_y), F32),
            pltpu.VMEM((4, slab_x, slab_y), F32),
        ),
        in_specs=[hbm] * 7,
        out_specs=(vmem, vmem),
        scratch_shapes=[
            pltpu.VMEM((props_count, parcels), F32),
            pltpu.VMEM((1, parcels), jnp.int32),
            pltpu.VMEM((1, parcels), jnp.int32),
            pltpu.VMEM((1, parcels), jnp.int32),
            pltpu.VMEM(class_table.shape, F32),
            pltpu.SMEM(class_table.shape, F32),
            pltpu.VMEM((5, slab_x, slab_y), F32),
            pltpu.VMEM((4, slab_x, slab_y), F32),
            pltpu.VMEM((4, slab_x, slab_y), F32),
            pltpu.VMEM((min(capacity, 256), parcels), F8),
            pltpu.VMEM((2 * ROWS, parcels), BF16),
            pltpu.VMEM((2 * ROWS, parcels), BF16),
            pltpu.VMEM((2, team, capacity // LANES * ROWS, LANES), F32),
            pltpu.VMEM((2, team * capacity // LANES * ROWS, LANES), F32),
            pltpu.VMEM((2 * slab_y, ROWS * capacity), F8),
            pltpu.VMEM((2, 4 * slab_x, 2 * slab_y), BF16),
            pltpu.VMEM((2, 2, 5 * slab_x, 2 * slab_y), F32),
            pltpu.VMEM((5, slab_x, slab_y), F32),
            pltpu.VMEM((5, slab_x, slab_y), F32),
            pltpu.VMEM((2, 2, ROWS, slab_y), F32),
            pltpu.VMEM((2, 2, ROWS, slab_y), F32),
            pltpu.VMEM((2, 2, ROWS, LANES), F32),
            pltpu.VMEM((2, 2, ROWS, LANES), F32),
            pltpu.SemaphoreType.DMA((8,)),
            pltpu.SemaphoreType.DMA((2,)),
            pltpu.SemaphoreType.DMA((2, team // ROWS)),
            pltpu.SemaphoreType.DMA((2,)),
            pltpu.SemaphoreType.DMA((2,)),
            pltpu.SemaphoreType.DMA((8,)),
        ],
        compiler_params=pltpu.CompilerParams(collective_id=0, has_side_effects=True),
    )(
        parcel_props,
        size_class.reshape(1, parcels),
        dest_owner.reshape(1, parcels),
        dest_local.reshape(1, parcels),
        class_table,
        gas_density,
        gas_rest,
    )
    return pl.pallas_call(
        store_kernel,
        out_shape=(
            jax.ShapeDtypeStruct(dens.shape, F32),
            jax.ShapeDtypeStruct(rest.shape, F32),
        ),
        in_specs=[hbm, hbm],
        out_specs=(hbm, hbm),
        scratch_shapes=[pltpu.SemaphoreType.DMA((2,))],
    )(*(pltpu.with_memory_space_constraint(x, pltpu.VMEM) for x in (dens, rest)))


def store_kernel(dens_ref, rest_ref, dens_out, rest_out, sem):
    stores = [
        pltpu.make_async_copy(dens_ref, dens_out, sem.at[0]),
        pltpu.make_async_copy(rest_ref, rest_out, sem.at[1]),
    ]
    for store in stores:
        store.start()
    for store in stores:
        store.wait()


def solution(mesh):
    return jax.shard_map(
        per_device,
        mesh=mesh,
        in_specs=(
            P(None, ("gx", "gy")),
            P(("gx", "gy")),
            P(("gx", "gy"), None),
            P(("gx", "gy")),
            P(),
            P("gx", "gy"),
            P(None, "gx", "gy"),
        ),
        out_specs=(P("gx", "gy"), P(None, "gx", "gy")),
        check_vma=False,
    )
```

```python
import functools

import jax
import jax.numpy as jnp
from jax import lax
from jax.experimental import pallas as pl
from jax.experimental.pallas import tpu as pltpu
from jax.sharding import PartitionSpec as P

F32 = jnp.float32
BF16 = jnp.bfloat16
F8 = jnp.float8_e4m3fn
LANES = 128
ROWS = 8
NT = (((1,), (1,)), ((), ()))
MESH = pl.DeviceIdType.MESH


def split(x):
    high = x.astype(BF16).astype(F32)
    return high, x - high


def pick(table, index, axis):
    other = (1 - axis,)
    return lax.gather(
        table,
        index[..., None],
        lax.GatherDimensionNumbers(
            offset_dims=(),
            collapsed_slice_dims=(axis,),
            start_index_map=(axis,),
            operand_batching_dims=other,
            start_indices_batching_dims=other,
        ),
        slice_sizes=(1, 1),
        mode=lax.GatherScatterMode.PROMISE_IN_BOUNDS,
    )


def iota(shape, dim):
    return lax.broadcasted_iota(jnp.int32, shape, dim)


def fused_kernel(
    width_x,
    width_y,
    capacity,
    props_hbm,
    class_hbm,
    owner_hbm,
    cell_hbm,
    table_hbm,
    dens_hbm,
    rest_hbm,
    dens_out,
    rest_out,
    props_ref,
    class_ref,
    owner_ref,
    cell_ref,
    table_ref,
    scalars_ref,
    field,
    flow,
    far_flow,
    hot,
    vals,
    keys,
    packed,
    got,
    spot,
    tab,
    total,
    far_out,
    far_in,
    row_out,
    row_in,
    col_out,
    col_in,
    load_sem,
    send_sem,
    recv_sem,
    far_send,
    far_recv,
    halo_recv,
):
    devices = width_x * width_y
    deep = width_x // 2
    team = deep * width_y
    groups = team // ROWS
    tiles = capacity // LANES
    block = tiles * ROWS
    my_x, my_y = lax.axis_index("gx"), lax.axis_index("gy")
    half = lax.div(my_x, deep)
    row_of = my_x - half * deep
    me = row_of * width_y + my_y
    base_x = half * deep
    mirror = (row_of + (1 - half) * deep, my_y)
    props_count, parcels = props_ref.shape
    classes = table_ref.shape[0]
    slab_x, slab_y = dens_hbm.shape

    def mate(local):
        return (base_x + lax.div(local, width_y), lax.rem(local, width_y))

    loads = [
        pltpu.make_async_copy(a, b, load_sem.at[i])
        for i, (a, b) in enumerate(
            [
                (owner_hbm, owner_ref),
                (dens_hbm, field.at[0]),
                (rest_hbm, field.at[1:5]),
                (table_hbm, table_ref),
                (class_hbm, class_ref),
                (cell_hbm, cell_ref),
                (props_hbm, props_ref),
                (table_hbm, scalars_ref),
            ]
        )
    ]
    for load in loads:
        load.start()

    barrier = pltpu.get_barrier_semaphore()

    def greet(target):
        pl.semaphore_signal(barrier, inc=1, device_id=target, device_id_type=MESH)

    def greet_mate(k, unused):
        greet(mate(lax.rem(me + k, team)))
        return unused

    middle = team // 2
    lax.fori_loop(middle, team, greet_mate, 0, unroll=True if team == 16 else 1)
    greet(mirror)
    last_low = (half == 0) & (row_of == deep - 1)
    first_high = (half == 1) & (row_of == 0)

    @pl.when(last_low)
    def _():
        greet((my_x + 1, my_y))

    @pl.when(first_high)
    def _():
        greet((my_x - 1, my_y))

    around = [
        ((mirror[0] + 1, my_y), row_of < deep - 1),
        ((mirror[0] - 1, my_y), row_of > 0),
        ((mirror[0], my_y + 1), my_y < width_y - 1),
        ((mirror[0], my_y - 1), my_y > 0),
    ]
    greets = team + jnp.where(last_low | first_high, 1, 0)
    for target, there in around:
        greets = greets + jnp.where(there, 1, 0)

        @pl.when(there)
        def _():
            greet(target)

    lax.fori_loop(1, middle, greet_mate, 0, unroll=True if team == 16 else 1)

    def rows_of(local):
        return pl.ds(pl.multiple_of(local * block, ROWS), block)

    def copy_to(phase, local):
        return pltpu.make_async_remote_copy(
            src_ref=packed.at[phase, local],
            dst_ref=got.at[phase, rows_of(me)],
            send_sem=send_sem.at[phase],
            recv_sem=recv_sem.at[phase, lax.div(me, ROWS)],
            device_id=mate(local),
            device_id_type=MESH,
        )

    def wait_blocks(phase, first, count):
        blocks = got.at[phase, pl.ds(pl.multiple_of(first * block, ROWS), count * block)]
        pltpu.make_async_remote_copy(
            src_ref=blocks,
            dst_ref=blocks,
            send_sem=send_sem.at[phase],
            recv_sem=recv_sem.at[phase, lax.div(first, ROWS)],
            device_id=mirror,
            device_id_type=MESH,
        ).wait_recv()

    def far_copy(out_ref, in_ref, i):
        return pltpu.make_async_remote_copy(
            src_ref=out_ref,
            dst_ref=in_ref,
            send_sem=far_send.at[i],
            recv_sem=far_recv.at[i],
            device_id=mirror,
            device_id_type=MESH,
        )

    loads[0].wait()
    row, col = (iota((LANES, 2 * LANES), 0), iota((LANES, 2 * LANES), 1))
    upper = jnp.where((col >= LANES) | (row < col), 1.0, 0.0).astype(BF16)
    ids = iota((devices, LANES), 0)
    wide = hot.shape[0]
    spans = capacity // wide
    ranks = iota((wide, LANES), 0).astype(F32).astype(BF16)
    one, zero = jnp.ones((), BF16), jnp.zeros((), BF16)
    carry = jnp.zeros((devices, LANES), F32)
    chunks = parcels // LANES
    for start in range(0, chunks, ROWS):
        span = range(start, min(start + ROWS, chunks))
        named = [owner_ref[:, c * LANES : (c + 1) * LANES] for c in span]
        mine = [jnp.where(owner == ids, 1.0, 0.0) for owner in named]
        counted = jnp.dot(
            jnp.concatenate(mine, axis=0).astype(BF16), upper, preferred_element_type=F32
        )
        for i, c in enumerate(span):
            part_of = counted[i * devices : (i + 1) * devices]
            rank = jnp.sum(mine[i] * (part_of[:, :LANES] + carry), axis=0, keepdims=True)
            carry = carry + part_of[:, LANES:]
            key = named[i].astype(F32)
            if spans > 1:
                level = sum(jnp.where(rank >= wide * k, 1.0, 0.0) for k in range(1, spans))
                rank = rank - level * wide
                key = key * spans + level
            at = slice(c * LANES, (c + 1) * LANES)
            keys[:, at] = jnp.broadcast_to(key, (2 * ROWS, LANES)).astype(BF16)
            hot[:, at] = jnp.where(ranks == rank.astype(BF16), one, zero).astype(F8)

    for load in loads[1:]:
        load.wait()
    inverse = 1.0 / field[0]
    for c in range(4):
        flow[c] = field[c + 1] * inverse
    eye = jnp.where(
        iota((props_count, props_count), 0) == iota((props_count, props_count), 1), 1.0, 0.0
    ).astype(BF16)
    table = jnp.concatenate(split(table_ref[...]), axis=0).astype(BF16)
    turned = lax.dot_general(eye, table, NT, preferred_element_type=F32).astype(BF16)
    picks = jnp.where(class_ref[...] == iota((classes, parcels), 0), 1.0, 0.0)
    picks = jnp.concatenate([picks, picks], axis=0).astype(BF16)
    coef = jnp.dot(turned, picks, preferred_element_type=F32)
    props = props_ref[...]
    which = iota((props_count, parcels), 0)
    weights = jnp.where(which >= 5, coef, jnp.where(which == 4, 1.0, 0.0))
    heat_sum = jnp.sum(weights * props, axis=0, keepdims=True)
    which = iota((ROWS, parcels), 0)
    mixed = jnp.where(which == 0, jnp.exp(0.5 * props[0:1]), props[0:ROWS])
    mixed = jnp.where(which == 5, heat_sum, mixed)
    mixed = jnp.where(which == 6, class_ref[...].astype(F32), mixed)
    mixed = jnp.where(which == 7, cell_ref[...].astype(F32), mixed)
    vals[...] = jnp.concatenate(split(mixed), axis=0).astype(BF16)

    def first_of(turn):
        return lax.rem(lax.div(me, ROWS) + turn, groups) * ROWS

    def pack(phase, turn):
        first = first_of(turn)
        first_id = jnp.where(phase == half, team, 0) + first
        count = ROWS * spans // 2
        both = [0.0, 0.0]
        for start in range(0, parcels, 256):
            at = slice(start, start + 256)
            for side in range(2):
                sends = [
                    jnp.where(
                        keys[:, at]
                        == (first_id * spans + side * count + i).astype(F32).astype(BF16),
                        vals[:, at],
                        zero,
                    )
                    for i in range(count)
                ]
                both[side] += lax.dot_general(
                    jnp.concatenate(sends, axis=0),
                    hot[:, at],
                    NT,
                    preferred_element_type=F32,
                )
        both = jnp.concatenate(both, axis=0)
        for i in range(ROWS):
            for k in range(spans):
                at = 2 * ROWS * (i * spans + k)
                whole = both[at : at + ROWS] + both[at + ROWS : at + 2 * ROWS]
                for t in range(wide // LANES):
                    tile = k * (wide // LANES) + t
                    packed[phase, first + i, tile * ROWS : (tile + 1) * ROWS] = whole[
                        :, t * LANES : (t + 1) * LANES
                    ]

    def launch(phase, turn, near):
        for i in range(1, ROWS if near else ROWS + 1):
            copy_to(phase, first_of(turn) + lax.rem(me + i, ROWS)).start()

    def send(phase, turn, near):
        pack(phase, turn)
        launch(phase, turn, near)

    def send_others(phase, start):
        if groups - start <= 2:
            for turn in range(start, groups):
                send(phase, turn, False)
        else:
            lax.fori_loop(start, groups, lambda k, u: (send(phase, k, False), u)[1], 0)

    early = row_of * 2 < deep
    low = jnp.where(half == 0, 1, 0)
    low_inner = jnp.where((half == 0) & jnp.logical_not(early), 1, 0)
    low_outer = low - low_inner
    pack(low_inner, 0)
    if groups > 1:
        pack(low_outer, 1)
    pl.semaphore_wait(barrier, greets)

    @pl.when(early)
    def _():
        far_copy(flow, far_flow, 0).start()

    launch(low_inner, 0, True)
    if groups > 1:
        launch(low_outer, 1, False)
        send_others(low_outer, 2)

    @pl.when(jnp.logical_not(early))
    def _():
        far_copy(flow, far_flow, 0).start()

    @pl.when(low_outer == 1)
    def _():
        send(1, 0, True)
        send_others(0, 1)

    @pl.when(low_outer == 0)
    def _():
        send_others(1, 1)
        send(1 - low_inner, 0, True)

    for phase in range(2):
        got[phase, rows_of(me)] = packed[phase, me]

    half_x = slab_x // 2
    ys = iota((2 * slab_y, capacity), 0).astype(F32).astype(BF16)
    xs_short = iota((half_x, capacity), 0).astype(F32).astype(BF16)
    sub = iota((ROWS, LANES), 0)

    def prepare(phase, fields):
        parts = []
        for c in range(4):
            for piece in split(fields[c]):
                parts.append(jnp.concatenate([piece[:half_x], piece[half_x:]], axis=1))
        tab[phase] = jnp.concatenate(parts, axis=0).astype(BF16)

    def take_group(phase, turn):
        if True:
            first = first_of(turn)

            @pl.when(turn == 0)
            def _():
                wait_blocks(phase, first, ROWS - 1)

            @pl.when(turn != 0)
            def _():
                wait_blocks(phase, first, ROWS)

            def part(c):
                return jnp.concatenate(
                    [
                        got[phase, pl.ds(first * block + t * ROWS + c, ROWS, stride=block), :]
                        for t in range(tiles)
                    ],
                    axis=1,
                )

            cell = part(7).astype(jnp.int32)
            line = lax.div(cell, slab_y)
            lane_of = cell - line * slab_y
            upper_half = jnp.where(line >= half_x, 1, 0)
            lanes_at = (lane_of + upper_half * slab_y).astype(F32)
            lines_short = (line - upper_half * half_x).astype(F32)
            line_at = line - upper_half * half_x
            shelf = lax.div(line_at, ROWS)
            within = line_at - shelf * ROWS
            gas = [[jnp.zeros((ROWS, LANES), F32)] * tiles for c in range(4)]
            for i in range(ROWS):
                spot_at = slice(i * capacity, (i + 1) * capacity)
                spot[:, spot_at] = jnp.where(
                    ys == lanes_at[i : i + 1].astype(BF16), one, zero
                ).astype(F8)
                found = jnp.dot(tab[phase], spot[:, spot_at], preferred_element_type=F32)
                for t in range(tiles):
                    lanes = slice(t * LANES, (t + 1) * LANES)
                    low, deep_row = [
                        jnp.broadcast_to(x[i : i + 1, lanes], (ROWS, LANES))
                        for x in (within, shelf)
                    ]
                    for c in range(4):
                        pieces = []
                        for p in range(2):
                            at = (2 * c + p) * half_x
                            piece = found[at : at + ROWS, lanes]
                            for r in range(1, half_x // ROWS):
                                here = found[at + r * ROWS : at + (r + 1) * ROWS, lanes]
                                piece = jnp.where(deep_row >= r, here, piece)
                            pieces.append(piece)
                        gas[c][t] = jnp.where(
                            sub == i, pick(pieces[0] + pieces[1], low, 0), gas[c][t]
                        )
            gas = [jnp.concatenate(row, axis=1) for row in gas]

            kind = part(6).astype(jnp.int32)
            coefs = [jnp.full(kind.shape, scalars_ref[0, j], F32) for j in range(5)]
            for k in range(1, classes):
                same = kind == k
                coefs = [jnp.where(same, scalars_ref[k, j], coefs[j]) for j in range(5)]
            mass = part(0)
            speed = [part(j) for j in (1, 2, 3)]
            heat, energy = part(4), part(5)
            slip = [speed[j] - gas[j] for j in range(3)]
            excess = heat - gas[3]
            soft = jnp.maximum(excess, 0.0) + jnp.log1p(jnp.exp(-jnp.abs(excess)))
            evapor = mass * (1.0 - jnp.exp(-(coefs[0] * soft)))
            square = slip[0] * slip[0] + slip[1] * slip[1] + slip[2] * slip[2]
            drag = mass * (1.0 - jnp.exp(-coefs[1] * jnp.sqrt(1.0 + square)))
            out = [evapor]
            out += [evapor * coefs[2 + j] * speed[j] + drag * slip[j] for j in range(3)]
            out += [evapor * energy]

            pieces = [piece for c in range(5) for piece in split(out[c])]
            spread = []
            for i in range(ROWS):
                in_row = xs_short == lines_short[i : i + 1].astype(BF16)
                spread.append(
                    jnp.concatenate(
                        [
                            jnp.where(in_row, piece[i : i + 1].astype(BF16), zero)
                            for piece in pieces
                        ],
                        axis=0,
                    )
                )
            for side in range(2):
                at = side * ROWS // 2
                total[phase, side] += lax.dot_general(
                    jnp.concatenate(spread[at : at + ROWS // 2], axis=1),
                    spot[:, at * capacity : (at + ROWS // 2) * capacity],
                    NT,
                    preferred_element_type=F32,
                )

    def deposit_of(phase):
        whole = total[phase, 0] + total[phase, 1]
        summed = []
        for c in range(5):
            at = 2 * c * half_x
            both = whole[at : at + half_x] + whole[at + half_x : at + 2 * half_x]
            summed.append(jnp.concatenate([both[:, :slab_y], both[:, slab_y:]], axis=0))
        return summed

    lane = iota((slab_x, slab_y), 1)
    line_id = iota((slab_x, slab_y), 0)

    def edges_of(origin):
        x, y = origin
        return [
            (row_out, row_in, 0, 0, (x - 1, y), x > 0, my_x < width_x - 1),
            (row_out, row_in, 1, 0, (x + 1, y), x < width_x - 1, my_x > 0),
            (col_out, col_in, 0, 2, (x, y - 1), y > 0, my_y < width_y - 1),
            (col_out, col_in, 1, 2, (x, y + 1), y < width_y - 1, my_y > 0),
        ]

    def edge(phase, out_ref, in_ref, side, base, target):
        at = 4 * phase + base + side
        return pltpu.make_async_remote_copy(
            src_ref=out_ref.at[phase, side],
            dst_ref=in_ref.at[phase, side],
            send_sem=load_sem.at[at],
            recv_sem=halo_recv.at[0],
            device_id=target,
            device_id_type=MESH,
        )

    origins = (mirror, (my_x, my_y))

    def send_edges(phase, deposit):
        sides = jnp.zeros((slab_x, slab_y), F32)
        for c in range(5):
            row_out[phase, 0, c : c + 1] = deposit[c][0:1]
            row_out[phase, 1, c : c + 1] = deposit[c][slab_x - 1 : slab_x]
            first = pltpu.roll(deposit[c], c, 1) if c else deposit[c]
            sides = jnp.where(lane == c, first, sides)
            last = pltpu.roll(deposit[c], ROWS + c + 1, 1)
            sides = jnp.where(lane == ROWS + c, last, sides)
        turned = jnp.transpose(sides)
        for side in range(2):
            col_out[phase, side, :, :slab_x] = turned[side * ROWS : (side + 1) * ROWS]
        for out_ref, in_ref, side, base, target, sends, takes in edges_of(origins[phase]):

            @pl.when(sends)
            def _():
                edge(phase, out_ref, in_ref, side, base, target).start()

    for ref in (row_out, col_out):
        ref[...] = jnp.zeros_like(ref)
    for out_ref, in_ref, side, base, target, sends, takes in edges_of(origins[1]):

        @pl.when(jnp.logical_not(takes))
        def _():
            for phase in range(2):
                in_ref[phase, side] = jnp.zeros(in_ref.shape[2:], F32)

    total[...] = jnp.zeros_like(total)
    prepare(1, flow)
    far_start = low_inner * groups
    far_stop = groups - 1 + low_outer + low_inner * groups
    own_stop = 2 * groups - 1 - low_inner * groups
    if groups == 1:
        far_stop, own_stop = low_inner, 1 - low_inner

    hold = jnp.where((half == 1) & jnp.logical_not(early), min(groups, 2), 0)

    def step(t, unused):
        head = (low_outer == 1) & (t < 2)
        ahead = jnp.where(t < groups + low_outer, 1, 0)
        far_turn = jnp.where(head, 1 - t, jnp.where(low_inner == 1, 1 - ahead, ahead))
        turn = jnp.where(head, 0, jnp.where(ahead == 1, t - low_outer, t - groups))

        @pl.when(t == far_start)
        def _():
            far_copy(flow, far_flow, 0).wait_recv()
            prepare(0, far_flow)

        take_group(1 - far_turn, turn)

        @pl.when(t == far_stop)
        def _():
            deposit = deposit_of(0)
            for c in range(5):
                far_out[c] = deposit[c]
            send_edges(0, deposit)

        @pl.when(t == own_stop)
        def _():
            send_edges(1, deposit_of(1))

        @pl.when(t == far_stop + hold)
        def _():
            far_copy(far_out, far_in, 1).start()

        return unused

    lax.fori_loop(0, 2 * groups, step, 0)
    mine = deposit_of(1)
    far_copy(far_out, far_in, 1).wait_recv()
    nothing = jnp.zeros((1, slab_y), F32)

    def out_of(c):
        return rest_out.at[c - 1] if c else dens_out

    for c in range(5):
        here = mine[c] + far_in[c]
        beside = jnp.concatenate([nothing, here[: slab_x - 1]], axis=0)
        beside += jnp.concatenate([here[1:], nothing], axis=0)
        beside += jnp.where(lane == 0, 0.0, pltpu.roll(here, 1, 1))
        beside += jnp.where(lane == slab_y - 1, 0.0, pltpu.roll(here, slab_y - 1, 1))
        out_of(c)[...] = field[c] + (0.4 * here + 0.15 * beside)

    takers = sum(jnp.where(takes, 1, 0) for *_, takes in edges_of(origins[1]))
    for count in range(1, 5):

        @pl.when(takers == count)
        def _():
            strips = got.at[0, pl.ds(0, 2 * count * ROWS)]
            pltpu.make_async_remote_copy(
                src_ref=strips,
                dst_ref=strips,
                send_sem=send_sem.at[0],
                recv_sem=halo_recv.at[0],
                device_id=mirror,
                device_id_type=MESH,
            ).wait_recv()

    rows_in = [0.15 * (row_in[0, side] + row_in[1, side]) for side in range(2)]
    cols_in = [
        jnp.transpose(0.15 * (col_in[0, side] + col_in[1, side]))[:slab_x]
        for side in range(2)
    ]
    for c in range(5):
        beside = [jnp.broadcast_to(x[:, c : c + 1], (slab_x, slab_y)) for x in cols_in]
        sides = jnp.where(
            lane == 0, beside[1], jnp.where(lane == slab_y - 1, beside[0], 0.0)
        )
        sides += jnp.where(line_id == 0, rows_in[1][c : c + 1], 0.0)
        sides += jnp.where(line_id == slab_x - 1, rows_in[0][c : c + 1], 0.0)
        out_of(c)[...] += sides

    for phase in range(2):
        blocks = packed.at[phase, pl.ds(0, team - 1)]
        pltpu.make_async_remote_copy(
            src_ref=blocks,
            dst_ref=blocks,
            send_sem=send_sem.at[phase],
            recv_sem=recv_sem.at[phase, 0],
            device_id=mirror,
            device_id_type=MESH,
        ).wait_send()
    far_copy(flow, far_flow, 0).wait_send()
    far_copy(far_out, far_in, 1).wait_send()
    for phase in range(2):
        for out_ref, in_ref, side, base, target, sends, takes in edges_of(origins[phase]):

            @pl.when(sends)
            def _():
                edge(phase, out_ref, in_ref, side, base, target).wait_send()


def per_device(
    parcel_props, size_class, dest_owner, dest_local, class_table, gas_density, gas_rest
):
    width_x, width_y = lax.axis_size("gx"), lax.axis_size("gy")
    devices = width_x * width_y
    team = devices // 2
    props_count, parcels = parcel_props.shape
    slab_x, slab_y = gas_density.shape
    capacity = -(-max(2, 4 * parcels // devices) // LANES) * LANES
    hbm = pl.BlockSpec(memory_space=pl.ANY)
    vmem = pl.BlockSpec(memory_space=pltpu.VMEM)
    dens, rest = pl.pallas_call(
        functools.partial(fused_kernel, width_x, width_y, capacity),
        out_shape=(
            pltpu.VMEM((slab_x, slab_y), F32),
            pltpu.VMEM((4, slab_x, slab_y), F32),
        ),
        in_specs=[hbm] * 7,
        out_specs=(vmem, vmem),
        scratch_shapes=[
            pltpu.VMEM((props_count, parcels), F32),
            pltpu.VMEM((1, parcels), jnp.int32),
            pltpu.VMEM((1, parcels), jnp.int32),
            pltpu.VMEM((1, parcels), jnp.int32),
            pltpu.VMEM(class_table.shape, F32),
            pltpu.SMEM(class_table.shape, F32),
            pltpu.VMEM((5, slab_x, slab_y), F32),
            pltpu.VMEM((4, slab_x, slab_y), F32),
            pltpu.VMEM((4, slab_x, slab_y), F32),
            pltpu.VMEM((min(capacity, 256), parcels), F8),
            pltpu.VMEM((2 * ROWS, parcels), BF16),
            pltpu.VMEM((2 * ROWS, parcels), BF16),
            pltpu.VMEM((2, team, capacity // LANES * ROWS, LANES), F32),
            pltpu.VMEM((2, team * capacity // LANES * ROWS, LANES), F32),
            pltpu.VMEM((2 * slab_y, ROWS * capacity), F8),
            pltpu.VMEM((2, 4 * slab_x, 2 * slab_y), BF16),
            pltpu.VMEM((2, 2, 5 * slab_x, 2 * slab_y), F32),
            pltpu.VMEM((5, slab_x, slab_y), F32),
            pltpu.VMEM((5, slab_x, slab_y), F32),
            pltpu.VMEM((2, 2, ROWS, slab_y), F32),
            pltpu.VMEM((2, 2, ROWS, slab_y), F32),
            pltpu.VMEM((2, 2, ROWS, LANES), F32),
            pltpu.VMEM((2, 2, ROWS, LANES), F32),
            pltpu.SemaphoreType.DMA((8,)),
            pltpu.SemaphoreType.DMA((2,)),
            pltpu.SemaphoreType.DMA((2, team // ROWS)),
            pltpu.SemaphoreType.DMA((2,)),
            pltpu.SemaphoreType.DMA((2,)),
            pltpu.SemaphoreType.DMA((1,)),
        ],
        compiler_params=pltpu.CompilerParams(collective_id=0, has_side_effects=True),
    )(
        parcel_props,
        size_class.reshape(1, parcels),
        dest_owner.reshape(1, parcels),
        dest_local.reshape(1, parcels),
        class_table,
        gas_density,
        gas_rest,
    )
    return pl.pallas_call(
        store_kernel,
        out_shape=(
            jax.ShapeDtypeStruct(dens.shape, F32),
            jax.ShapeDtypeStruct(rest.shape, F32),
        ),
        in_specs=[hbm, hbm],
        out_specs=(hbm, hbm),
        scratch_shapes=[pltpu.SemaphoreType.DMA((2,))],
    )(*(pltpu.with_memory_space_constraint(x, pltpu.VMEM) for x in (dens, rest)))


def store_kernel(dens_ref, rest_ref, dens_out, rest_out, sem):
    stores = [
        pltpu.make_async_copy(dens_ref, dens_out, sem.at[0]),
        pltpu.make_async_copy(rest_ref, rest_out, sem.at[1]),
    ]
    for store in stores:
        store.start()
    for store in stores:
        store.wait()


def solution(mesh):
    return jax.shard_map(
        per_device,
        mesh=mesh,
        in_specs=(
            P(None, ("gx", "gy")),
            P(("gx", "gy")),
            P(("gx", "gy"), None),
            P(("gx", "gy")),
            P(),
            P("gx", "gy"),
            P(None, "gx", "gy"),
        ),
        out_specs=(P("gx", "gy"), P(None, "gx", "gy")),
        check_vma=False,
    )
```

```python
import functools

import jax
import jax.numpy as jnp
from jax import lax
from jax.experimental import pallas as pl
from jax.experimental.pallas import tpu as pltpu
from jax.sharding import PartitionSpec as P

F32 = jnp.float32
BF16 = jnp.bfloat16
F8 = jnp.float8_e4m3fn
LANES = 128
ROWS = 8
NT = (((1,), (1,)), ((), ()))
MESH = pl.DeviceIdType.MESH


def split(x):
    high = x.astype(BF16).astype(F32)
    return high, x - high


def pick(table, index, axis):
    other = (1 - axis,)
    return lax.gather(
        table,
        index[..., None],
        lax.GatherDimensionNumbers(
            offset_dims=(),
            collapsed_slice_dims=(axis,),
            start_index_map=(axis,),
            operand_batching_dims=other,
            start_indices_batching_dims=other,
        ),
        slice_sizes=(1, 1),
        mode=lax.GatherScatterMode.PROMISE_IN_BOUNDS,
    )


def iota(shape, dim):
    return lax.broadcasted_iota(jnp.int32, shape, dim)


def fused_kernel(
    width_x,
    width_y,
    capacity,
    props_hbm,
    class_hbm,
    owner_hbm,
    cell_hbm,
    table_hbm,
    dens_hbm,
    rest_hbm,
    dens_out,
    rest_out,
    props_ref,
    class_ref,
    owner_ref,
    cell_ref,
    table_ref,
    scalars_ref,
    field,
    flow,
    far_flow,
    hot,
    vals,
    keys,
    packed,
    got,
    spot,
    tab,
    total,
    far_out,
    far_in,
    row_out,
    row_in,
    col_out,
    col_in,
    load_sem,
    send_sem,
    recv_sem,
    far_send,
    far_recv,
    halo_recv,
):
    devices = width_x * width_y
    deep = width_x // 2
    team = deep * width_y
    groups = team // ROWS
    tiles = capacity // LANES
    block = tiles * ROWS
    my_x, my_y = lax.axis_index("gx"), lax.axis_index("gy")
    half = lax.div(my_x, deep)
    row_of = my_x - half * deep
    me = row_of * width_y + my_y
    base_x = half * deep
    mirror = (row_of + (1 - half) * deep, my_y)
    props_count, parcels = props_ref.shape
    classes = table_ref.shape[0]
    slab_x, slab_y = dens_hbm.shape

    def mate(local):
        return (base_x + lax.div(local, width_y), lax.rem(local, width_y))

    loads = [
        pltpu.make_async_copy(a, b, load_sem.at[i])
        for i, (a, b) in enumerate(
            [
                (owner_hbm, owner_ref),
                (dens_hbm, field.at[0]),
                (rest_hbm, field.at[1:5]),
                (table_hbm, table_ref),
                (class_hbm, class_ref),
                (cell_hbm, cell_ref),
                (props_hbm, props_ref),
                (table_hbm, scalars_ref),
            ]
        )
    ]
    for load in loads:
        load.start()

    barrier = pltpu.get_barrier_semaphore()

    def greet(target):
        pl.semaphore_signal(barrier, inc=1, device_id=target, device_id_type=MESH)

    def greet_mate(k, unused):
        greet(mate(lax.rem(me + k, team)))
        return unused

    middle = team // 2
    lax.fori_loop(middle, team, greet_mate, 0, unroll=True if team == 16 else 1)
    greet(mirror)
    last_low = (half == 0) & (row_of == deep - 1)
    first_high = (half == 1) & (row_of == 0)

    @pl.when(last_low)
    def _():
        greet((my_x + 1, my_y))

    @pl.when(first_high)
    def _():
        greet((my_x - 1, my_y))

    around = [
        ((mirror[0] + 1, my_y), row_of < deep - 1),
        ((mirror[0] - 1, my_y), row_of > 0),
        ((mirror[0], my_y + 1), my_y < width_y - 1),
        ((mirror[0], my_y - 1), my_y > 0),
    ]
    greets = team + jnp.where(last_low | first_high, 1, 0)
    for target, there in around:
        greets = greets + jnp.where(there, 1, 0)

        @pl.when(there)
        def _():
            greet(target)

    lax.fori_loop(1, middle, greet_mate, 0, unroll=True if team == 16 else 1)

    def rows_of(local):
        return pl.ds(pl.multiple_of(local * block, ROWS), block)

    def copy_to(phase, local):
        return pltpu.make_async_remote_copy(
            src_ref=packed.at[phase, local],
            dst_ref=got.at[phase, rows_of(me)],
            send_sem=send_sem.at[phase],
            recv_sem=recv_sem.at[phase, lax.div(me, ROWS)],
            device_id=mate(local),
            device_id_type=MESH,
        )

    def wait_blocks(phase, first, count):
        blocks = got.at[phase, pl.ds(pl.multiple_of(first * block, ROWS), count * block)]
        pltpu.make_async_remote_copy(
            src_ref=blocks,
            dst_ref=blocks,
            send_sem=send_sem.at[phase],
            recv_sem=recv_sem.at[phase, lax.div(first, ROWS)],
            device_id=mirror,
            device_id_type=MESH,
        ).wait_recv()

    def far_copy(out_ref, in_ref, i):
        return pltpu.make_async_remote_copy(
            src_ref=out_ref,
            dst_ref=in_ref,
            send_sem=far_send.at[i],
            recv_sem=far_recv.at[i],
            device_id=mirror,
            device_id_type=MESH,
        )

    loads[0].wait()
    row, col = (iota((LANES, 2 * LANES), 0), iota((LANES, 2 * LANES), 1))
    upper = jnp.where((col >= LANES) | (row < col), 1.0, 0.0).astype(BF16)
    ids = iota((devices, LANES), 0)
    wide = hot.shape[0]
    spans = capacity // wide
    ranks = iota((wide, LANES), 0).astype(F32).astype(BF16)
    one, zero = jnp.ones((), BF16), jnp.zeros((), BF16)
    carry = jnp.zeros((devices, LANES), F32)
    chunks = parcels // LANES
    for start in range(0, chunks, ROWS):
        span = range(start, min(start + ROWS, chunks))
        named = [owner_ref[:, c * LANES : (c + 1) * LANES] for c in span]
        mine = [jnp.where(owner == ids, 1.0, 0.0) for owner in named]
        counted = jnp.dot(
            jnp.concatenate(mine, axis=0).astype(BF16), upper, preferred_element_type=F32
        )
        for i, c in enumerate(span):
            part_of = counted[i * devices : (i + 1) * devices]
            rank = jnp.sum(mine[i] * (part_of[:, :LANES] + carry), axis=0, keepdims=True)
            carry = carry + part_of[:, LANES:]
            key = named[i].astype(F32)
            if spans > 1:
                level = sum(jnp.where(rank >= wide * k, 1.0, 0.0) for k in range(1, spans))
                rank = rank - level * wide
                key = key * spans + level
            at = slice(c * LANES, (c + 1) * LANES)
            keys[:, at] = jnp.broadcast_to(key, (2 * ROWS, LANES)).astype(BF16)
            hot[:, at] = jnp.where(ranks == rank.astype(BF16), one, zero).astype(F8)

    for load in loads[1:]:
        load.wait()
    inverse = 1.0 / field[0]
    for c in range(4):
        flow[c] = field[c + 1] * inverse
    eye = jnp.where(
        iota((props_count, props_count), 0) == iota((props_count, props_count), 1), 1.0, 0.0
    ).astype(BF16)
    table = jnp.concatenate(split(table_ref[...]), axis=0).astype(BF16)
    turned = lax.dot_general(eye, table, NT, preferred_element_type=F32).astype(BF16)
    picks = jnp.where(class_ref[...] == iota((classes, parcels), 0), 1.0, 0.0)
    picks = jnp.concatenate([picks, picks], axis=0).astype(BF16)
    coef = jnp.dot(turned, picks, preferred_element_type=F32)
    props = props_ref[...]
    which = iota((props_count, parcels), 0)
    weights = jnp.where(which >= 5, coef, jnp.where(which == 4, 1.0, 0.0))
    heat_sum = jnp.sum(weights * props, axis=0, keepdims=True)
    which = iota((ROWS, parcels), 0)
    mixed = jnp.where(which == 0, jnp.exp(0.5 * props[0:1]), props[0:ROWS])
    mixed = jnp.where(which == 5, heat_sum, mixed)
    mixed = jnp.where(which == 6, class_ref[...].astype(F32), mixed)
    mixed = jnp.where(which == 7, cell_ref[...].astype(F32), mixed)
    vals[...] = jnp.concatenate(split(mixed), axis=0).astype(BF16)

    def first_of(turn):
        return lax.rem(lax.div(me, ROWS) + turn, groups) * ROWS

    def pack(phase, turn):
        first = first_of(turn)
        first_id = jnp.where(phase == half, team, 0) + first
        count = ROWS * spans // 2
        both = [0.0, 0.0]
        for start in range(0, parcels, 256):
            at = slice(start, start + 256)
            for side in range(2):
                sends = [
                    jnp.where(
                        keys[:, at]
                        == (first_id * spans + side * count + i).astype(F32).astype(BF16),
                        vals[:, at],
                        zero,
                    )
                    for i in range(count)
                ]
                both[side] += lax.dot_general(
                    jnp.concatenate(sends, axis=0),
                    hot[:, at],
                    NT,
                    preferred_element_type=F32,
                )
        both = jnp.concatenate(both, axis=0)
        for i in range(ROWS):
            for k in range(spans):
                at = 2 * ROWS * (i * spans + k)
                whole = both[at : at + ROWS] + both[at + ROWS : at + 2 * ROWS]
                for t in range(wide // LANES):
                    tile = k * (wide // LANES) + t
                    packed[phase, first + i, tile * ROWS : (tile + 1) * ROWS] = whole[
                        :, t * LANES : (t + 1) * LANES
                    ]

    def launch(phase, turn, near):
        for i in range(1, ROWS if near else ROWS + 1):
            copy_to(phase, first_of(turn) + lax.rem(me + i, ROWS)).start()

    def send(phase, turn, near):
        pack(phase, turn)
        launch(phase, turn, near)

    def send_others(phase, start):
        if groups - start <= 2:
            for turn in range(start, groups):
                send(phase, turn, False)
        else:
            lax.fori_loop(start, groups, lambda k, u: (send(phase, k, False), u)[1], 0)

    early = row_of * 2 < deep
    low = jnp.where(half == 0, 1, 0)
    low_inner = jnp.where((half == 0) & jnp.logical_not(early), 1, 0)
    low_outer = low - low_inner
    pack(low_inner, 0)
    if groups > 1:
        pack(low_outer, 1)
    pl.semaphore_wait(barrier, greets)

    @pl.when(early)
    def _():
        far_copy(flow, far_flow, 0).start()

    launch(low_inner, 0, True)
    if groups > 1:
        launch(low_outer, 1, False)
        send_others(low_outer, 2)

    @pl.when(jnp.logical_not(early))
    def _():
        far_copy(flow, far_flow, 0).start()

    @pl.when(low_outer == 1)
    def _():
        send(1, 0, True)
        send_others(0, 1)

    @pl.when(low_outer == 0)
    def _():
        send_others(1, 1)
        send(1 - low_inner, 0, True)

    for phase in range(2):
        got[phase, rows_of(me)] = packed[phase, me]

    half_x = slab_x // 2
    ys = iota((2 * slab_y, capacity), 0).astype(F32).astype(BF16)
    xs_short = iota((half_x, capacity), 0).astype(F32).astype(BF16)
    sub = iota((ROWS, LANES), 0)

    def prepare(phase, fields):
        parts = []
        for c in range(4):
            for piece in split(fields[c]):
                parts.append(jnp.concatenate([piece[:half_x], piece[half_x:]], axis=1))
        tab[phase] = jnp.concatenate(parts, axis=0).astype(BF16)

    def take_group(phase, turn):
        if True:
            first = first_of(turn)

            @pl.when(turn == 0)
            def _():
                wait_blocks(phase, first, ROWS - 1)

            @pl.when(turn != 0)
            def _():
                wait_blocks(phase, first, ROWS)

            def part(c):
                return jnp.concatenate(
                    [
                        got[phase, pl.ds(first * block + t * ROWS + c, ROWS, stride=block), :]
                        for t in range(tiles)
                    ],
                    axis=1,
                )

            cell = part(7).astype(jnp.int32)
            line = lax.div(cell, slab_y)
            lane_of = cell - line * slab_y
            upper_half = jnp.where(line >= half_x, 1, 0)
            lanes_at = (lane_of + upper_half * slab_y).astype(F32)
            lines_short = (line - upper_half * half_x).astype(F32)
            line_at = line - upper_half * half_x
            shelf = lax.div(line_at, ROWS)
            within = line_at - shelf * ROWS
            gas = [[jnp.zeros((ROWS, LANES), F32)] * tiles for c in range(4)]
            for i in range(ROWS):
                spot_at = slice(i * capacity, (i + 1) * capacity)
                spot[:, spot_at] = jnp.where(
                    ys == lanes_at[i : i + 1].astype(BF16), one, zero
                ).astype(F8)
                found = jnp.dot(tab[phase], spot[:, spot_at], preferred_element_type=F32)
                for t in range(tiles):
                    lanes = slice(t * LANES, (t + 1) * LANES)
                    low, deep_row = [
                        jnp.broadcast_to(x[i : i + 1, lanes], (ROWS, LANES))
                        for x in (within, shelf)
                    ]
                    for c in range(4):
                        pieces = []
                        for p in range(2):
                            at = (2 * c + p) * half_x
                            piece = found[at : at + ROWS, lanes]
                            for r in range(1, half_x // ROWS):
                                here = found[at + r * ROWS : at + (r + 1) * ROWS, lanes]
                                piece = jnp.where(deep_row >= r, here, piece)
                            pieces.append(piece)
                        gas[c][t] = jnp.where(
                            sub == i, pick(pieces[0] + pieces[1], low, 0), gas[c][t]
                        )
            gas = [jnp.concatenate(row, axis=1) for row in gas]

            kind = part(6).astype(jnp.int32)
            coefs = [jnp.full(kind.shape, scalars_ref[0, j], F32) for j in range(5)]
            for k in range(1, classes):
                same = kind == k
                coefs = [jnp.where(same, scalars_ref[k, j], coefs[j]) for j in range(5)]
            mass = part(0)
            speed = [part(j) for j in (1, 2, 3)]
            heat, energy = part(4), part(5)
            slip = [speed[j] - gas[j] for j in range(3)]
            excess = heat - gas[3]
            soft = jnp.maximum(excess, 0.0) + jnp.log1p(jnp.exp(-jnp.abs(excess)))
            evapor = mass * (1.0 - jnp.exp(-(coefs[0] * soft)))
            square = slip[0] * slip[0] + slip[1] * slip[1] + slip[2] * slip[2]
            drag = mass * (1.0 - jnp.exp(-coefs[1] * jnp.sqrt(1.0 + square)))
            out = [evapor]
            out += [evapor * coefs[2 + j] * speed[j] + drag * slip[j] for j in range(3)]
            out += [evapor * energy]

            pieces = [piece for c in range(5) for piece in split(out[c])]
            spread = []
            for i in range(ROWS):
                in_row = xs_short == lines_short[i : i + 1].astype(BF16)
                spread.append(
                    jnp.concatenate(
                        [
                            jnp.where(in_row, piece[i : i + 1].astype(BF16), zero)
                            for piece in pieces
                        ],
                        axis=0,
                    )
                )
            for side in range(2):
                at = side * ROWS // 2
                total[phase, side] += lax.dot_general(
                    jnp.concatenate(spread[at : at + ROWS // 2], axis=1),
                    spot[:, at * capacity : (at + ROWS // 2) * capacity],
                    NT,
                    preferred_element_type=F32,
                )

    def deposit_of(phase):
        whole = total[phase, 0] + total[phase, 1]
        summed = []
        for c in range(5):
            at = 2 * c * half_x
            both = whole[at : at + half_x] + whole[at + half_x : at + 2 * half_x]
            summed.append(jnp.concatenate([both[:, :slab_y], both[:, slab_y:]], axis=0))
        return summed

    lane = iota((slab_x, slab_y), 1)
    line_id = iota((slab_x, slab_y), 0)

    def edges_of(origin):
        x, y = origin
        return [
            (row_out, row_in, 0, 0, (x - 1, y), x > 0, my_x < width_x - 1),
            (row_out, row_in, 1, 0, (x + 1, y), x < width_x - 1, my_x > 0),
            (col_out, col_in, 0, 2, (x, y - 1), y > 0, my_y < width_y - 1),
            (col_out, col_in, 1, 2, (x, y + 1), y < width_y - 1, my_y > 0),
        ]

    def edge(phase, out_ref, in_ref, side, base, target):
        at = 4 * phase + base + side
        return pltpu.make_async_remote_copy(
            src_ref=out_ref.at[phase, side],
            dst_ref=in_ref.at[phase, side],
            send_sem=load_sem.at[at],
            recv_sem=halo_recv.at[0],
            device_id=target,
            device_id_type=MESH,
        )

    origins = (mirror, (my_x, my_y))

    def send_edges(phase, deposit):
        sides = jnp.zeros((slab_x, slab_y), F32)
        for c in range(5):
            row_out[phase, 0, c : c + 1] = deposit[c][0:1]
            row_out[phase, 1, c : c + 1] = deposit[c][slab_x - 1 : slab_x]
            first = pltpu.roll(deposit[c], c, 1) if c else deposit[c]
            sides = jnp.where(lane == c, first, sides)
            last = pltpu.roll(deposit[c], ROWS + c + 1, 1)
            sides = jnp.where(lane == ROWS + c, last, sides)
        turned = jnp.transpose(sides)
        for side in range(2):
            col_out[phase, side, :, :slab_x] = turned[side * ROWS : (side + 1) * ROWS]
        for out_ref, in_ref, side, base, target, sends, takes in edges_of(origins[phase]):

            @pl.when(sends)
            def _():
                edge(phase, out_ref, in_ref, side, base, target).start()

    for ref in (row_out, col_out):
        ref[...] = jnp.zeros_like(ref)
    for out_ref, in_ref, side, base, target, sends, takes in edges_of(origins[1]):

        @pl.when(jnp.logical_not(takes))
        def _():
            for phase in range(2):
                in_ref[phase, side] = jnp.zeros(in_ref.shape[2:], F32)

    total[...] = jnp.zeros_like(total)
    prepare(1, flow)
    far_start = low_inner * groups
    far_stop = groups - 1 + low_outer + low_inner * groups
    own_stop = 2 * groups - 1 - low_inner * groups
    if groups == 1:
        far_stop, own_stop = low_inner, 1 - low_inner

    hold = jnp.where((half == 1) & jnp.logical_not(early), min(groups, 2), 0)

    def step(t, unused):
        head = (low_outer == 1) & (t < 2)
        ahead = jnp.where(t < groups + low_outer, 1, 0)
        far_turn = jnp.where(head, 1 - t, jnp.where(low_inner == 1, 1 - ahead, ahead))
        turn = jnp.where(head, 0, jnp.where(ahead == 1, t - low_outer, t - groups))

        @pl.when(t == far_start)
        def _():
            far_copy(flow, far_flow, 0).wait_recv()
            prepare(0, far_flow)

        take_group(1 - far_turn, turn)

        @pl.when(t == far_stop)
        def _():
            deposit = deposit_of(0)
            for c in range(5):
                far_out[c] = deposit[c]
            send_edges(0, deposit)

        @pl.when(t == far_stop + hold)
        def _():
            far_copy(far_out, far_in, 1).start()

        @pl.when(t == own_stop)
        def _():
            send_edges(1, deposit_of(1))

        return unused

    lax.fori_loop(0, 2 * groups, step, 0)
    mine = deposit_of(1)
    far_copy(far_out, far_in, 1).wait_recv()
    nothing = jnp.zeros((1, slab_y), F32)

    def out_of(c):
        return rest_out.at[c - 1] if c else dens_out

    for c in range(5):
        here = mine[c] + far_in[c]
        beside = jnp.concatenate([nothing, here[: slab_x - 1]], axis=0)
        beside += jnp.concatenate([here[1:], nothing], axis=0)
        beside += jnp.where(lane == 0, 0.0, pltpu.roll(here, 1, 1))
        beside += jnp.where(lane == slab_y - 1, 0.0, pltpu.roll(here, slab_y - 1, 1))
        out_of(c)[...] = field[c] + (0.4 * here + 0.15 * beside)

    takers = sum(jnp.where(takes, 1, 0) for *_, takes in edges_of(origins[1]))
    for count in range(1, 5):

        @pl.when(takers == count)
        def _():
            strips = got.at[0, pl.ds(0, 2 * count * ROWS)]
            pltpu.make_async_remote_copy(
                src_ref=strips,
                dst_ref=strips,
                send_sem=send_sem.at[0],
                recv_sem=halo_recv.at[0],
                device_id=mirror,
                device_id_type=MESH,
            ).wait_recv()

    rows_in = [0.15 * (row_in[0, side] + row_in[1, side]) for side in range(2)]
    cols_in = [
        jnp.transpose(0.15 * (col_in[0, side] + col_in[1, side]))[:slab_x]
        for side in range(2)
    ]
    for c in range(5):
        beside = [jnp.broadcast_to(x[:, c : c + 1], (slab_x, slab_y)) for x in cols_in]
        sides = jnp.where(
            lane == 0, beside[1], jnp.where(lane == slab_y - 1, beside[0], 0.0)
        )
        sides += jnp.where(line_id == 0, rows_in[1][c : c + 1], 0.0)
        sides += jnp.where(line_id == slab_x - 1, rows_in[0][c : c + 1], 0.0)
        out_of(c)[...] += sides

    for phase in range(2):
        blocks = packed.at[phase, pl.ds(0, team - 1)]
        pltpu.make_async_remote_copy(
            src_ref=blocks,
            dst_ref=blocks,
            send_sem=send_sem.at[phase],
            recv_sem=recv_sem.at[phase, 0],
            device_id=mirror,
            device_id_type=MESH,
        ).wait_send()
    far_copy(flow, far_flow, 0).wait_send()
    far_copy(far_out, far_in, 1).wait_send()
    for phase in range(2):
        for out_ref, in_ref, side, base, target, sends, takes in edges_of(origins[phase]):

            @pl.when(sends)
            def _():
                edge(phase, out_ref, in_ref, side, base, target).wait_send()


def per_device(
    parcel_props, size_class, dest_owner, dest_local, class_table, gas_density, gas_rest
):
    width_x, width_y = lax.axis_size("gx"), lax.axis_size("gy")
    devices = width_x * width_y
    team = devices // 2
    props_count, parcels = parcel_props.shape
    slab_x, slab_y = gas_density.shape
    capacity = -(-max(2, 4 * parcels // devices) // LANES) * LANES
    hbm = pl.BlockSpec(memory_space=pl.ANY)
    vmem = pl.BlockSpec(memory_space=pltpu.VMEM)
    dens, rest = pl.pallas_call(
        functools.partial(fused_kernel, width_x, width_y, capacity),
        out_shape=(
            pltpu.VMEM((slab_x, slab_y), F32),
            pltpu.VMEM((4, slab_x, slab_y), F32),
        ),
        in_specs=[hbm] * 7,
        out_specs=(vmem, vmem),
        scratch_shapes=[
            pltpu.VMEM((props_count, parcels), F32),
            pltpu.VMEM((1, parcels), jnp.int32),
            pltpu.VMEM((1, parcels), jnp.int32),
            pltpu.VMEM((1, parcels), jnp.int32),
            pltpu.VMEM(class_table.shape, F32),
            pltpu.SMEM(class_table.shape, F32),
            pltpu.VMEM((5, slab_x, slab_y), F32),
            pltpu.VMEM((4, slab_x, slab_y), F32),
            pltpu.VMEM((4, slab_x, slab_y), F32),
            pltpu.VMEM((min(capacity, 256), parcels), F8),
            pltpu.VMEM((2 * ROWS, parcels), BF16),
            pltpu.VMEM((2 * ROWS, parcels), BF16),
            pltpu.VMEM((2, team, capacity // LANES * ROWS, LANES), F32),
            pltpu.VMEM((2, team * capacity // LANES * ROWS, LANES), F32),
            pltpu.VMEM((2 * slab_y, ROWS * capacity), F8),
            pltpu.VMEM((2, 4 * slab_x, 2 * slab_y), BF16),
            pltpu.VMEM((2, 2, 5 * slab_x, 2 * slab_y), F32),
            pltpu.VMEM((5, slab_x, slab_y), F32),
            pltpu.VMEM((5, slab_x, slab_y), F32),
            pltpu.VMEM((2, 2, ROWS, slab_y), F32),
            pltpu.VMEM((2, 2, ROWS, slab_y), F32),
            pltpu.VMEM((2, 2, ROWS, LANES), F32),
            pltpu.VMEM((2, 2, ROWS, LANES), F32),
            pltpu.SemaphoreType.DMA((8,)),
            pltpu.SemaphoreType.DMA((2,)),
            pltpu.SemaphoreType.DMA((2, team // ROWS)),
            pltpu.SemaphoreType.DMA((2,)),
            pltpu.SemaphoreType.DMA((2,)),
            pltpu.SemaphoreType.DMA((1,)),
        ],
        compiler_params=pltpu.CompilerParams(collective_id=0, has_side_effects=True),
    )(
        parcel_props,
        size_class.reshape(1, parcels),
        dest_owner.reshape(1, parcels),
        dest_local.reshape(1, parcels),
        class_table,
        gas_density,
        gas_rest,
    )
    return pl.pallas_call(
        store_kernel,
        out_shape=(
            jax.ShapeDtypeStruct(dens.shape, F32),
            jax.ShapeDtypeStruct(rest.shape, F32),
        ),
        in_specs=[hbm, hbm],
        out_specs=(hbm, hbm),
        scratch_shapes=[pltpu.SemaphoreType.DMA((2,))],
    )(*(pltpu.with_memory_space_constraint(x, pltpu.VMEM) for x in (dens, rest)))


def store_kernel(dens_ref, rest_ref, dens_out, rest_out, sem):
    stores = [
        pltpu.make_async_copy(dens_ref, dens_out, sem.at[0]),
        pltpu.make_async_copy(rest_ref, rest_out, sem.at[1]),
    ]
    for store in stores:
        store.start()
    for store in stores:
        store.wait()


def solution(mesh):
    return jax.shard_map(
        per_device,
        mesh=mesh,
        in_specs=(
            P(None, ("gx", "gy")),
            P(("gx", "gy")),
            P(("gx", "gy"), None),
            P(("gx", "gy")),
            P(),
            P("gx", "gy"),
            P(None, "gx", "gy"),
        ),
        out_specs=(P("gx", "gy"), P(None, "gx", "gy")),
        check_vma=False,
    )
```
